512 devices in a mesh: seq: 32 (over z, x), mp: 16 (over y, core).
Axes of the slice: x: 4, y: 8, z: 8, core: 2. Of those that a mesh axis runs over, the one named last changes fastest.
Arguments:
- inputs: bfloat16 [16384, 4096], P('seq', 'mp'), may hold values from -6 to 6
- guess: float32 [16384, 2, 2048], P('seq', None, 'mp'), may hold values from -4 to 4
- initial: float32 [2, 2048], P(None, 'mp'), may hold values from -4 to 4
- w_in: bfloat16 [4096, 2, 2048], P(None, None, 'mp'), may hold values from -0.09375 to 0.09375
- bias: float32 [2, 2048], P(None, 'mp'), may hold values from -3 to 3
- angle: float32 [2048], P('mp'), may hold values from -3.140625 to 3.140625
- strength: float32 [2048], P('mp'), may hold values from 0 to 1, as said below
- w_out: bfloat16 [2, 2048, 4096], P(None, 'mp'), may hold values from -0.09375 to 0.09375
Outputs:
- new_state: float32 [16384, 2, 2048], P('seq', None, 'mp')
- output: bfloat16 [16384, 4096], P('seq', 'mp')
The draws below stay inside these ranges and needn't reach their ends.
Inputs may be any that keep to these rules, and one draw needn't show every extreme that they name: `strength`: each pair's nonlinear weight; every value lies either between 0.3 and 1 (strongly nonlinear pairs) or between 0.1 / 16384 and 1 / 16384 (pairs nearly linear over the whole sequence), in any mix.
All inputs are finite; a program needn't handle non-finite values.
Results may differ from the reference program's by a relative error of at most 0.018.
Values may be sent and summed in bfloat16 or wider, within the bound.
A program may use at most 64 MiB of HBM per device.

```python
import jax
import jax.numpy as jnp
from jax import lax

D = 4096
HALF = 2048
TOKENS = 16384
N_MP = 16


def draw_strength(key, part):
    pick_key, fast_key, slow_key = jax.random.split(jax.random.fold_in(key, 17), 3)
    fast_share = 0.5
    is_fast = jax.random.uniform(pick_key, (HALF,), jnp.float32) < fast_share
    fast_value = jax.random.uniform(fast_key, (HALF,), jnp.float32, 0.3, 1.0)
    slow_exponent = jax.random.uniform(slow_key, (HALF,), jnp.float32, jnp.log(0.1), 0.0)
    slow_value = jnp.exp(slow_exponent) / TOKENS
    return jnp.where(is_fast, fast_value, slow_value).astype(jnp.float32)


def level_of(own_key, dims, cuts, smallest, largest):
    factor_of = 1.0
    for position, shards_of in cuts:
        draws = jax.random.uniform(jax.random.fold_in(jax.random.fold_in(own_key, 6), position), (shards_of,), jnp.float32, smallest / len(cuts), largest / len(cuts))
        factor_of = factor_of * jnp.repeat(jnp.exp(draws), dims[position] // shards_of).reshape((-1,) + (1,) * (len(dims) - 1 - position))
    return factor_of


def noise(own_key, dims, deviation, most, cuts=(), held_as=jnp.bfloat16):
    array = jax.random.normal(own_key, dims, jnp.float32) * deviation
    if len(cuts) > 0:
        array = level_of(own_key, dims, cuts, -0.22, 0.18) * array
    return jnp.clip(array, min=-most, max=most).astype(held_as)


def setup_inputs(seed: int = 0) -> dict:
    key_of = jax.random.split(jax.random.key(seed), 9)
    inputs = noise(key_of[0], (TOKENS, D), 1.0, 6.0, ((0, 32), (1, 16)))
    guess = noise(key_of[1], (TOKENS, 2, HALF), 0.5, 4.0, ((0, 32), (2, 16)), jnp.float32)
    initial = noise(key_of[2], (2, HALF), 1.0, 4.0, ((1, 16),), jnp.float32)
    w_in = noise(key_of[3], (D, 2, HALF), D ** -0.5, 0.09375, ((2, 16),))
    bias = noise(key_of[4], (2, HALF), 0.5, 3.0, ((1, 16),), jnp.float32)
    angle = jnp.clip(jax.random.uniform(key_of[5], (HALF,), jnp.float32, -3.140625, 3.140625), -3.140625, 3.140625)
    strength = draw_strength(jax.random.fold_in(key_of[8], 71), 0)
    w_out = noise(key_of[7], (2, HALF, D), D ** -0.5, 0.09375, ((1, 16),))
    return {"inputs": inputs, "guess": guess, "initial": initial, "w_in": w_in, "bias": bias, "angle": angle, "strength": strength, "w_out": w_out}


def linearize(previous, drive, angle, strength):
    cosine = jnp.cos(angle)
    sine = jnp.sin(angle)
    first = cosine * previous[:, 0] - sine * previous[:, 1]
    second = sine * previous[:, 0] + cosine * previous[:, 1]
    squash_one = jnp.tanh(first + drive[:, 0])
    squash_two = jnp.tanh(second + drive[:, 1])
    value_one = first + strength * (squash_one - first)
    value_two = second + strength * (squash_two - second)
    slope_one = 1.0 - strength * squash_one * squash_one
    slope_two = 1.0 - strength * squash_two * squash_two
    jac_aa = slope_one * cosine
    jac_ab = -slope_one * sine
    jac_ba = slope_two * sine
    jac_bb = slope_two * cosine
    offset_one = value_one - (jac_aa * previous[:, 0] + jac_ab * previous[:, 1])
    offset_two = value_two - (jac_ba * previous[:, 0] + jac_bb * previous[:, 1])
    return (jac_aa, jac_ab, jac_ba, jac_bb, offset_one, offset_two)


def advance(state, terms):
    jac_aa, jac_ab, jac_ba, jac_bb, offset_one, offset_two = terms
    first = jac_aa * state[0] + jac_ab * state[1] + offset_one
    second = jac_ba * state[0] + jac_bb * state[1] + offset_two
    result = jnp.stack([first, second])
    return result, result


def reference(inputs, guess, initial, w_in, bias, angle, strength, w_out):
    width = inputs.shape[1]
    steps_all = inputs.shape[0]
    pairs = initial.shape[1]
    drive = jnp.dot(inputs, w_in.reshape(width, 2 * pairs), preferred_element_type=jnp.float32)
    drive = drive.reshape(steps_all, 2, pairs) + bias[None]
    previous = jnp.concatenate([initial[None], guess[:-1]], axis=0)
    terms = linearize(previous, drive, angle, strength)
    _, new_state = lax.scan(advance, initial, terms)
    group = pairs // N_MP
    grouped_state = new_state.astype(jnp.bfloat16).reshape(steps_all, 2, N_MP, group)
    grouped_out = w_out.reshape(2, N_MP, group, width)

    def add_group(member, total):
        state_part = lax.dynamic_index_in_dim(grouped_state, member, 2, keepdims=False).reshape(steps_all, 2 * group)
        weight_part = lax.dynamic_index_in_dim(grouped_out, member, 1, keepdims=False).reshape(2 * group, width)
        partial_value = jnp.dot(state_part, weight_part, preferred_element_type=jnp.float32).astype(jnp.bfloat16)
        return total + partial_value.astype(jnp.float32)

    total = lax.fori_loop(0, N_MP, add_group, jnp.zeros((steps_all, width), jnp.float32))
    return new_state, total.astype(jnp.bfloat16)
```

```python
import jax
import jax.numpy as jnp
from jax import lax
from jax.experimental import pallas as pl
from jax.experimental.pallas import tpu as pltpu
from jax.sharding import PartitionSpec as P

MESH = pl.DeviceIdType.MESH
F32 = jnp.float32
BF16 = jnp.bfloat16

NY = 8
NX = 4
NZ = 8
NS = NX * NZ
ROWS = 512
BLK = 256
Q = 4
CH = ROWS // Q
SEG = CH // 8
STEPS = 14


def compose(later, earlier):
    a, b, c, d, e, f = later
    p, q, r, s, t, u = earlier
    return (
        a * p + b * r,
        a * q + b * s,
        c * p + d * r,
        c * q + d * s,
        a * t + b * u + e,
        c * t + d * u + f,
    )


def apply_map(m, state):
    a, b, c, d, e, f = m
    x, y = state
    return (a * x + b * y + e, c * x + d * y + f)


def kernel(
    x_hbm,
    g_hbm,
    init_hbm,
    w_hbm,
    bias_hbm,
    ang_hbm,
    str_hbm,
    wo_hbm,
    nsb,
    outb,
    xg,
    w2,
    wi,
    wtmp,
    wo,
    acc,
    gs,
    rot,
    terms,
    seg,
    tot,
    xbuf,
    rowtot,
    zbuf,
    stb,
    sbuf,
    rbuf,
    otmp,
    ini,
    bia,
    ang,
    stg,
    loc_sem,
    agi_recv,
    agd_recv,
    ag_send,
    d2d_send,
    g_sem,
    wo_sem,
    x_send,
    x_recv,
    z_send,
    z_recv,
    st_send,
    st_recv,
    rs_send,
    rs_recv,
):
    s = lax.axis_index("seq")
    m = lax.axis_index("mp")
    y = m // 2
    c = m % 2
    zi = s // NX
    xi = s % NX

    def ring(k):
        return lax.rem(y + k + 2 * NY, NY)

    def dev(seq, mp):
        return {"seq": seq, "mp": mp}

    up = dev(s, ring(1) * 2 + c)
    down = dev(s, ring(-1) * 2 + c)
    partner = dev(s, y * 2 + 1 - c)

    in_copy = pltpu.make_async_copy(x_hbm, xg.at[m], loc_sem.at[0])
    in_copy.start()
    w_copy = pltpu.make_async_copy(w_hbm, w2, loc_sem.at[1])
    w_copy.start()
    g_copy = pltpu.make_async_copy(g_hbm, gs.at[pl.ds(8, 2 * ROWS)], loc_sem.at[2])
    g_copy.start()
    small = [
        pltpu.make_async_copy(a, b, loc_sem.at[3 + i])
        for i, (a, b) in enumerate(
            ((init_hbm, ini), (bias_hbm, bia), (ang_hbm, ang), (str_hbm, stg))
        )
    ]
    for copy in small:
        copy.start()

    barrier = pltpu.get_barrier_semaphore()

    def greet(target):
        pl.semaphore_signal(barrier, inc=1, device_id=target, device_id_type=MESH)

    for target in (up, down, partner):
        greet(target)
    for dx in range(1, NX):
        greet(dev(zi * NX + lax.rem(xi + dx, NX), m))
    for dz in range(1, NZ):
        greet(dev(lax.rem(zi + dz, NZ) * NX + xi, m))
    greet(dev(lax.rem(s + 1, NS), m))
    greet(dev(lax.rem(s + NS - 1, NS), m))
    pl.semaphore_wait(barrier, 3 + (NX - 1) + (NZ - 1) + 2)

    def rows(q):
        return pl.ds(pl.multiple_of(q * CH, CH), CH)

    def ici(block, q, g, d, half):
        ref = xg.at[block, rows(q)]
        if half:
            ref = xg.at[block, rows(q), pl.ds(d * (BLK // 2), BLK // 2)]
        return pltpu.make_async_remote_copy(
            src_ref=ref,
            dst_ref=ref,
            send_sem=ag_send.at[0],
            recv_sem=agi_recv.at[d, g, q],
            device_id=(up, down)[d],
            device_id_type=MESH,
        )

    def d2d(block, q, g, d, half):
        ref = xg.at[block, rows(q)]
        if half:
            ref = xg.at[block, rows(q), pl.ds(d * (BLK // 2), BLK // 2)]
        return pltpu.make_async_remote_copy(
            src_ref=ref,
            dst_ref=ref,
            send_sem=d2d_send.at[0],
            recv_sem=agd_recv.at[d, g, q],
            device_id=partner,
            device_id_type=MESH,
        )

    in_copy.wait()
    for q in range(Q):
        for d in range(2):
            ici(m, q, 0, d, False).start()
    for q in range(Q):
        d2d(m, q, 0, 0, False).start()

    g_send = pltpu.make_async_remote_copy(
        src_ref=g_hbm.at[pl.ds(2 * ROWS - 8, 8)],
        dst_ref=gs.at[pl.ds(0, 8)],
        send_sem=g_sem.at[0],
        recv_sem=g_sem.at[1],
        device_id=dev(lax.rem(s + 1, NS), m),
        device_id_type=MESH,
    )

    @pl.when(s < NS - 1)
    def _():
        g_send.start()

    def wo_cols(k, core):
        return wo_hbm.at[:, pl.ds(pl.multiple_of((2 * k + core) * BLK, BLK), BLK)]

    for k in range(NY):
        pltpu.make_async_copy(wo_cols(k, c), wo.at[c, k], wo_sem.at[0]).start()
        pltpu.make_async_remote_copy(
            src_ref=wo_cols(k, 1 - c),
            dst_ref=wo.at[c, k],
            send_sem=wo_sem.at[1],
            recv_sem=wo_sem.at[2],
            device_id=partner,
            device_id_type=MESH,
        ).start()

    w_copy.wait()

    @pl.loop(0, 16)
    def _(b):
        wtmp[...] = w2[pl.ds(pl.multiple_of(b * 2 * BLK, 2 * BLK), 2 * BLK), :].astype(F32)
        for k in range(2):
            wi[b, :, k * 128 : (k + 1) * 128] = wtmp[pl.ds(k, BLK, stride=2), :].astype(BF16)

    for copy in small:
        copy.wait()
    cosine = jnp.broadcast_to(jnp.cos(ang[...]), (8, 128))
    sine = jnp.broadcast_to(jnp.sin(ang[...]), (8, 128))
    strength = jnp.broadcast_to(stg[...], (8, 128))

    bias_row = jnp.concatenate([bia[0:1, :], bia[1:2, :]], axis=1)
    other = y * 2 + 1 - c

    @pl.loop(0, Q)
    def _(q):
        d2d(other, q, 0, 0, False).wait_recv()
        r = rows(q)
        part = jnp.dot(xg[m, r, :], wi[m], preferred_element_type=F32)
        part += jnp.dot(xg[other, r, :], wi[other], preferred_element_type=F32)
        part += bias_row
        acc[0, r, :] = part[:, :128]
        acc[1, r, :] = part[:, 128:]

    def rotate_guess():
        g_copy.wait()

        @pl.when(s > 0)
        def _():
            g_send.wait_recv()

        @pl.when(s == 0)
        def _():
            gs[6:8, :] = ini[...]

        for q in range(Q):

            @pl.loop(0, SEG)
            def _(j):
                at = 6 + 2 * (q * CH + j)
                one = gs[pl.ds(at, 8, stride=2 * SEG), :]
                two = gs[pl.ds(at + 1, 8, stride=2 * SEG), :]
                rot[q, j, 0] = cosine * one - sine * two
                rot[q, j, 1] = sine * one + cosine * two

    def add_group(g, q):
        r = rows(q)
        part = None
        for d in range(2):
            pos = ring(-g if d == 0 else g)
            d2d(2 * pos + 1 - c, q, g, d, False).wait_recv()
            for core in range(2):
                b = 2 * pos + core
                term = jnp.dot(xg[b, r, :], wi[b], preferred_element_type=F32)
                part = term if part is None else part + term
        acc[0, r, :] += part[:, :128]
        acc[1, r, :] += part[:, 128:]

    for g in range(1, 4):

        @pl.loop(0, Q)
        def _(q):
            for d in range(2):
                b = 2 * ring(-g if d == 0 else g) + c
                ici(b, q, g - 1, d, False).wait_recv()
                ici(b, q, g, d, g == 3).start()
                d2d(b, q, g, d, False).start()
            if g > 1:
                add_group(g - 1, q)

        if g == 1:
            rotate_guess()

    @pl.loop(0, Q)
    def _(q):
        add_group(3, q)

    iota = lax.broadcasted_iota(jnp.int32, (8, 128), 0)
    one_v = jnp.ones((8, 128), F32)
    zero_v = jnp.zeros((8, 128), F32)
    identity = (one_v, zero_v, zero_v, one_v, zero_v, zero_v)

    def shifted(mm, k):
        return tuple(
            jnp.where(iota < k, ident, pltpu.roll(v, k, 0)) for v, ident in zip(mm, identity)
        )

    far = ring(4)

    @pl.loop(0, Q)
    def _(q):
        b = 2 * far + c
        for d in range(2):
            ici(b, q, 3, d, True).wait_recv()
            d2d(b, q, 4, d, True).start()
        r = rows(q)
        part = jnp.dot(xg[b, r, :], wi[b], preferred_element_type=F32)
        b2 = 2 * far + 1 - c
        for d in range(2):
            d2d(b2, q, 4, d, True).wait_recv()
        part += jnp.dot(xg[b2, r, :], wi[b2], preferred_element_type=F32)
        acc[0, r, :] += part[:, :128]
        acc[1, r, :] += part[:, 128:]
        mm = None
        for j in range(SEG):
            at = q * CH + j
            r1 = rot[q, j, 0]
            r2 = rot[q, j, 1]
            sq1 = jnp.tanh(r1 + acc[0, pl.ds(at, 8, stride=SEG), :])
            sq2 = jnp.tanh(r2 + acc[1, pl.ds(at, 8, stride=SEG), :])
            t1 = sq1 * sq1
            t2 = sq2 * sq2
            sl1 = 1.0 - strength * t1
            sl2 = 1.0 - strength * t2
            of1 = strength * (sq1 - r1 * (1.0 - t1))
            of2 = strength * (sq2 - r2 * (1.0 - t2))
            terms[q, j, 0] = sl1
            terms[q, j, 1] = sl2
            terms[q, j, 2] = of1
            terms[q, j, 3] = of2
            here = (sl1 * cosine, -sl1 * sine, sl2 * sine, sl2 * cosine, of1, of2)
            mm = here if mm is None else compose(here, mm)
        for k in (1, 2, 4):
            mm = compose(mm, shifted(mm, k))
        before = shifted(mm, 1)
        for i in range(6):
            seg[q, i] = before[i]
            seg[q, 6 + i] = jnp.broadcast_to(mm[i][7:8, :], (8, 128))

    def chunk_total(q):
        return tuple(seg[q, 6 + i] for i in range(6))

    whole = chunk_total(0)
    for q in range(1, Q):
        whole = compose(chunk_total(q), whole)
    for i in range(6):
        tot[i : i + 1, :] = whole[i][0:1, :]
    for i in range(6, 8):
        tot[i : i + 1, :] = jnp.zeros((1, 128), F32)

    def x_copy(dx):
        return pltpu.make_async_remote_copy(
            src_ref=tot,
            dst_ref=xbuf.at[dx],
            send_sem=x_send.at[dx],
            recv_sem=x_recv.at[dx],
            device_id=dev(zi * NX + lax.rem(xi + dx, NX), m),
            device_id_type=MESH,
        )

    for dx in range(1, NX):
        x_copy(dx).start()
    for dx in range(1, NX):
        x_copy(dx).wait_recv()

    def from_x(k):
        def member(i):
            value = whole[i]
            for dx in range(1, NX):
                here = lax.rem(xi - k + NX, NX) == dx
                value = jnp.where(here, jnp.broadcast_to(xbuf[dx, i : i + 1, :], (8, 128)), value)
            return value

        return tuple(member(i) for i in range(6))

    line = from_x(0)
    ahead = tuple(jnp.where(xi > 0, v, ident) for v, ident in zip(line, identity))
    for k in range(1, NX):
        mk = from_x(k)
        line = compose(mk, line)
        if k < NX - 1:
            more = compose(mk, ahead)
            ahead = tuple(jnp.where(xi > k, v, w) for v, w in zip(more, ahead))
    for i in range(6):
        rowtot[i : i + 1, :] = line[i][0:1, :]
    for i in range(6, 8):
        rowtot[i : i + 1, :] = jnp.zeros((1, 128), F32)

    def z_copy(dz):
        return pltpu.make_async_remote_copy(
            src_ref=rowtot,
            dst_ref=zbuf.at[dz],
            send_sem=z_send.at[dz],
            recv_sem=z_recv.at[dz],
            device_id=dev(lax.rem(zi + dz, NZ) * NX + xi, m),
            device_id_type=MESH,
        )

    for dz in range(1, NZ):

        @pl.when(zi + dz < NZ)
        def _():
            z_copy(dz).start()

    for dz in range(1, NZ):

        @pl.when(zi >= dz)
        def _():
            z_copy(dz).wait_recv()

    state = tuple(jnp.broadcast_to(ini[k : k + 1, :], (8, 128)) for k in range(2))
    for dz in range(NZ - 1, 0, -1):
        mk = tuple(jnp.broadcast_to(zbuf[dz, i : i + 1, :], (8, 128)) for i in range(6))
        after = apply_map(mk, state)
        state = tuple(jnp.where(zi >= dz, v, w) for v, w in zip(after, state))
    state = apply_map(ahead, state)

    entering = [state]
    for q in range(Q - 1):
        entering.append(apply_map(chunk_total(q), entering[-1]))
    current = [
        apply_map(tuple(seg[q, i] for i in range(6)), entering[q]) for q in range(Q)
    ]

    def st_copy(q, core):
        return pltpu.make_async_remote_copy(
            src_ref=stb.at[core, q],
            dst_ref=stb.at[core, q],
            send_sem=st_send.at[q],
            recv_sem=st_recv.at[q],
            device_id=partner,
            device_id_type=MESH,
        )

    for q in range(Q):
        pair = [[], []]
        x1, x2 = current[q]
        for j in range(SEG):
            u1 = cosine * x1 - sine * x2
            u2 = sine * x1 + cosine * x2
            x1 = terms[q, j, 0] * u1 + terms[q, j, 2]
            x2 = terms[q, j, 1] * u2 + terms[q, j, 3]
            at = 2 * (q * CH + j)
            nsb[pl.ds(at, 8, stride=2 * SEG), :] = x1
            nsb[pl.ds(at + 1, 8, stride=2 * SEG), :] = x2
            pair[0].append(x1)
            pair[1].append(x2)
            if j % 2 == 1:
                for k in range(2):
                    both = jnp.concatenate(pair[k], axis=0).astype(BF16)
                    stb[c, q, (j - 1) * 8 : (j + 1) * 8, k * 128 : (k + 1) * 128] = both
                pair = [[], []]
        st_copy(q, c).start()

    pltpu.make_async_copy(wo.at[c], wo.at[c], wo_sem.at[0]).wait()
    wo_all = pltpu.make_async_remote_copy(
        src_ref=wo.at[1 - c],
        dst_ref=wo.at[1 - c],
        send_sem=wo_sem.at[1],
        recv_sem=wo_sem.at[2],
        device_id=partner,
        device_id_type=MESH,
    )
    wo_all.wait_recv()
    for q in range(Q):
        st_copy(q, 1 - c).wait_recv()

    def own(k, q):
        part = jnp.dot(stb[0, q], wo[0, k], preferred_element_type=F32)
        return part + jnp.dot(stb[1, q], wo[1, k], preferred_element_type=F32)

    def rs_copy(d, i):
        return pltpu.make_async_remote_copy(
            src_ref=sbuf.at[d, i],
            dst_ref=rbuf.at[d, i],
            send_sem=rs_send.at[0],
            recv_sem=rs_recv.at[d, i],
            device_id=(up, down)[d],
            device_id_type=MESH,
        )

    @pl.loop(0, 4)
    def _(i):
        for d in range(2):
            dist = (17 - i) // 4
            k = ring(dist) if d == 0 else ring(-dist)
            q = lax.rem(i + 2 * d, Q)
            sbuf[d, i] = own(k, q).astype(BF16)
            rs_copy(d, i).start()

    @pl.loop(4, STEPS)
    def _(i):
        for d in range(2):
            dist = (17 - i) // 4
            k = ring(dist) if d == 0 else ring(-dist)
            q = lax.rem(i + 2 * d, Q)
            mine = own(k, q)
            rs_copy(d, i - 4).wait_recv()
            sbuf[d, i] = (mine + rbuf[d, i - 4].astype(F32)).astype(BF16)
            rs_copy(d, i).start()

    for q in (2, 0, 3, 1):
        mine = own(y, q)
        up_at = 10 + (q + 2) % 4
        down_at = 10 + q
        rs_copy(0, up_at).wait_recv()
        rs_copy(1, down_at).wait_recv()
        total = mine + rbuf[0, up_at].astype(F32) + rbuf[1, down_at].astype(F32)
        for j in range(SEG):
            for h in range(2):
                otmp[h, pl.ds(j, 8, stride=SEG), :] = total[
                    j * 8 : (j + 1) * 8, h * 128 : (h + 1) * 128
                ]
        for h in range(2):
            outb[q * CH : (q + 1) * CH, h * 128 : (h + 1) * 128] = otmp[h].astype(BF16)

    def sent(ref, sem):
        pltpu.make_async_remote_copy(
            src_ref=ref,
            dst_ref=ref,
            send_sem=sem,
            recv_sem=rs_recv.at[0, 0],
            device_id=partner,
            device_id_type=MESH,
        ).wait_send()

    sent(xg.at[pl.ds(0, 7)], ag_send.at[0])
    sent(xg.at[pl.ds(0, 8)], d2d_send.at[0])
    sent(sbuf, rs_send.at[0])
    wo_all.wait_send()

    @pl.when(s < NS - 1)
    def _():
        g_send.wait_send()

    for dx in range(1, NX):
        x_copy(dx).wait_send()
    for dz in range(1, NZ):

        @pl.when(zi + dz < NZ)
        def _():
            z_copy(dz).wait_send()

    for q in range(Q):
        st_copy(q, c).wait_send()


def local(inputs, guess, initial, w_in, bias, angle, strength, w_out):
    dma = pltpu.SemaphoreType.DMA
    hbm = pl.BlockSpec(memory_space=pltpu.HBM)
    vmem = pl.BlockSpec(memory_space=pltpu.VMEM)
    new_state, output = pl.pallas_call(
        kernel,
        out_shape=(
            jax.ShapeDtypeStruct((2 * ROWS, 128), F32),
            jax.ShapeDtypeStruct((ROWS, BLK), BF16),
        ),
        in_specs=[hbm] * 8,
        out_specs=(vmem, vmem),
        scratch_shapes=[
            pltpu.VMEM((16, ROWS, BLK), BF16),
            pltpu.VMEM((8192, 128), BF16),
            pltpu.VMEM((16, BLK, BLK), BF16),
            pltpu.VMEM((2 * BLK, 128), F32),
            pltpu.VMEM((2, NY, BLK, BLK), BF16),
            pltpu.VMEM((2, ROWS, 128), F32),
            pltpu.VMEM((8 + 2 * ROWS, 128), F32),
            pltpu.VMEM((Q, SEG, 2, 8, 128), F32),
            pltpu.VMEM((Q, SEG, 4, 8, 128), F32),
            pltpu.VMEM((Q, 12, 8, 128), F32),
            pltpu.VMEM((8, 128), F32),
            pltpu.VMEM((NX, 8, 128), F32),
            pltpu.VMEM((8, 128), F32),
            pltpu.VMEM((NZ, 8, 128), F32),
            pltpu.VMEM((2, Q, CH, BLK), BF16),
            pltpu.VMEM((2, STEPS, CH, BLK), BF16),
            pltpu.VMEM((2, STEPS, CH, BLK), BF16),
            pltpu.VMEM((2, CH, 128), F32),
            pltpu.VMEM((2, 128), F32),
            pltpu.VMEM((2, 128), F32),
            pltpu.VMEM((1, 128), F32),
            pltpu.VMEM((1, 128), F32),
            dma((7,)),
            dma((2, 4, Q)),
            dma((2, 5, Q)),
            dma((1,)),
            dma((1,)),
            dma((2,)),
            dma((3,)),
            dma((NX,)),
            dma((NX,)),
            dma((NZ,)),
            dma((NZ,)),
            dma((Q,)),
            dma((Q,)),
            dma((1,)),
            dma((2, STEPS)),
        ],
        compiler_params=pltpu.CompilerParams(
            collective_id=0, has_side_effects=True, vmem_limit_bytes=48 * 1024 * 1024
        ),
    )(*(pltpu.with_memory_space_constraint(v, pltpu.HBM) for v in (
        inputs,
        guess.reshape(2 * ROWS, 128),
        initial,
        w_in.reshape(8192, 128),
        bias,
        angle.reshape(1, 128),
        strength.reshape(1, 128),
        w_out.reshape(BLK, 4096),
    )))
    return new_state.reshape(ROWS, 2, 128), output


def solution(mesh):
    placed = (
        P("seq", "mp"),
        P("seq", None, "mp"),
        P(None, "mp"),
        P(None, None, "mp"),
        P(None, "mp"),
        P("mp"),
        P("mp"),
        P(None, "mp", None),
    )
    return jax.shard_map(
        local,
        mesh=mesh,
        in_specs=placed,
        out_specs=(P("seq", None, "mp"), P("seq", "mp")),
        check_vma=False,
    )
```

```python
import jax
import jax.numpy as jnp
from jax import lax
from jax.experimental import pallas as pl
from jax.experimental.pallas import tpu as pltpu
from jax.sharding import PartitionSpec as P

MESH = pl.DeviceIdType.MESH
F32 = jnp.float32
BF16 = jnp.bfloat16

NY = 8
NX = 4
NZ = 8
NS = NX * NZ
ROWS = 512
BLK = 256
Q = 4
CH = ROWS // Q
SEG = CH // 8
STEPS = 14


def compose(later, earlier):
    a, b, c, d, e, f = later
    p, q, r, s, t, u = earlier
    return (
        a * p + b * r,
        a * q + b * s,
        c * p + d * r,
        c * q + d * s,
        a * t + b * u + e,
        c * t + d * u + f,
    )


def apply_map(m, state):
    a, b, c, d, e, f = m
    x, y = state
    return (a * x + b * y + e, c * x + d * y + f)


def kernel(
    x_hbm,
    g_hbm,
    init_hbm,
    w_hbm,
    bias_hbm,
    ang_hbm,
    str_hbm,
    wo_hbm,
    nsb,
    outb,
    xg,
    w2,
    wi,
    wtmp,
    wo,
    acc,
    gs,
    rot,
    terms,
    seg,
    tot,
    xbuf,
    rowtot,
    zbuf,
    stb,
    sbuf,
    rbuf,
    otmp,
    ini,
    bia,
    ang,
    stg,
    loc_sem,
    agi_recv,
    agd_recv,
    ag_send,
    d2d_send,
    g_sem,
    wo_sem,
    x_send,
    x_recv,
    z_send,
    z_recv,
    st_send,
    st_recv,
    rs_send,
    rs_recv,
    ready,
):
    s = lax.axis_index("seq")
    m = lax.axis_index("mp")
    y = m // 2
    c = m % 2
    zi = s // NX
    xi = s % NX

    def ring(k):
        return lax.rem(y + k + 2 * NY, NY)

    def dev(seq, mp):
        return {"seq": seq, "mp": mp}

    up = dev(s, ring(1) * 2 + c)
    down = dev(s, ring(-1) * 2 + c)
    partner = dev(s, y * 2 + 1 - c)

    in_copy = pltpu.make_async_copy(x_hbm, xg.at[m], loc_sem.at[0])
    in_copy.start()
    w_copy = pltpu.make_async_copy(w_hbm, w2, loc_sem.at[1])
    w_copy.start()
    g_copy = pltpu.make_async_copy(g_hbm, gs.at[pl.ds(8, 2 * ROWS)], loc_sem.at[2])
    g_copy.start()
    small = [
        pltpu.make_async_copy(a, b, loc_sem.at[3 + i])
        for i, (a, b) in enumerate(
            ((init_hbm, ini), (bias_hbm, bia), (ang_hbm, ang), (str_hbm, stg))
        )
    ]
    for copy in small:
        copy.start()

    barrier = pltpu.get_barrier_semaphore()

    def greet(target):
        pl.semaphore_signal(barrier, inc=1, device_id=target, device_id_type=MESH)

    for target in (up, down, partner):
        greet(target)
    for dx in range(1, NX):

        @pl.when(xi + dx < NX)
        def _():
            greet(dev(s + dx, m))

    for dz in range(1, NZ):

        @pl.when(zi + dz < NZ)
        def _():
            greet(dev(s + dz * NX, m))

    @pl.when(s < NS - 1)
    def _():
        greet(dev(s + 1, m))

    pl.semaphore_wait(barrier, 3 + xi + zi + lax.min(s, 1))

    def answer(sem, target):
        pl.semaphore_signal(sem, inc=1, device_id=target, device_id_type=MESH)

    @pl.when(s > 0)
    def _():
        answer(ready.at[0], dev(s - 1, m))

    for dx in range(1, NX):

        @pl.when(xi >= dx)
        def _():
            answer(ready.at[1], dev(s - dx, m))

    for dz in range(1, NZ):

        @pl.when(zi >= dz)
        def _():
            answer(ready.at[2], dev(s - dz * NX, m))

    def rows(q):
        return pl.ds(pl.multiple_of(q * CH, CH), CH)

    def ici(block, q, g, d, half):
        ref = xg.at[block, rows(q)]
        if half:
            ref = xg.at[block, rows(q), pl.ds(d * (BLK // 2), BLK // 2)]
        return pltpu.make_async_remote_copy(
            src_ref=ref,
            dst_ref=ref,
            send_sem=ag_send.at[0],
            recv_sem=agi_recv.at[d, g, q],
            device_id=(up, down)[d],
            device_id_type=MESH,
        )

    def d2d(block, q, g, d, half):
        ref = xg.at[block, rows(q)]
        if half:
            ref = xg.at[block, rows(q), pl.ds(d * (BLK // 2), BLK // 2)]
        return pltpu.make_async_remote_copy(
            src_ref=ref,
            dst_ref=ref,
            send_sem=d2d_send.at[0],
            recv_sem=agd_recv.at[d, g, q],
            device_id=partner,
            device_id_type=MESH,
        )

    in_copy.wait()
    for q in range(Q):
        for d in range(2):
            ici(m, q, 0, d, False).start()
    for q in range(Q):
        d2d(m, q, 0, 0, False).start()

    g_send = pltpu.make_async_remote_copy(
        src_ref=g_hbm.at[pl.ds(2 * ROWS - 8, 8)],
        dst_ref=gs.at[pl.ds(0, 8)],
        send_sem=g_sem.at[0],
        recv_sem=g_sem.at[1],
        device_id=dev(lax.rem(s + 1, NS), m),
        device_id_type=MESH,
    )

    def wo_cols(k, core):
        return wo_hbm.at[:, pl.ds(pl.multiple_of((2 * k + core) * BLK, BLK), BLK)]

    for k in range(NY):
        pltpu.make_async_copy(wo_cols(k, c), wo.at[c, k], wo_sem.at[0]).start()
        pltpu.make_async_remote_copy(
            src_ref=wo_cols(k, 1 - c),
            dst_ref=wo.at[c, k],
            send_sem=wo_sem.at[1],
            recv_sem=wo_sem.at[2],
            device_id=partner,
            device_id_type=MESH,
        ).start()

    def prepare(b):
        wtmp[...] = w2[pl.ds(pl.multiple_of(b * 2 * BLK, 2 * BLK), 2 * BLK), :].astype(F32)
        for k in range(2):
            wi[b, :, k * 128 : (k + 1) * 128] = wtmp[pl.ds(k, BLK, stride=2), :].astype(BF16)

    other = y * 2 + 1 - c
    far = ring(4)
    w_copy.wait()

    @pl.loop(0, 4)
    def _(i):
        prepare(2 * ring((i // 2) * 4) + lax.rem(i, 2))

    for copy in small:
        copy.wait()
    cosine = jnp.broadcast_to(jnp.cos(ang[...]), (8, 128))
    sine = jnp.broadcast_to(jnp.sin(ang[...]), (8, 128))
    strength = jnp.broadcast_to(stg[...], (8, 128))
    bias_row = jnp.concatenate([bia[0:1, :], bia[1:2, :]], axis=1)

    def start_group(q):
        d2d(other, q, 0, 0, False).wait_recv()
        r = rows(q)
        part = jnp.dot(xg[m, r, :], wi[m], preferred_element_type=F32)
        part += jnp.dot(xg[other, r, :], wi[other], preferred_element_type=F32)
        part += bias_row
        acc[0, r, :] = part[:, :128]
        acc[1, r, :] = part[:, 128:]

    def rotate_guess(q):
        @pl.loop(0, SEG)
        def _(j):
            at = 6 + 2 * (q * CH + j)
            one = gs[pl.ds(at, 8, stride=2 * SEG), :]
            two = gs[pl.ds(at + 1, 8, stride=2 * SEG), :]
            rot[q, j, 0] = cosine * one - sine * two
            rot[q, j, 1] = sine * one + cosine * two

    def add_group(g, q):
        r = rows(q)
        part = None
        for d in range(2):
            pos = ring(-g if d == 0 else g)
            d2d(2 * pos + 1 - c, q, g, d, False).wait_recv()
            for core in range(2):
                b = 2 * pos + core
                term = jnp.dot(xg[b, r, :], wi[b], preferred_element_type=F32)
                part = term if part is None else part + term
        acc[0, r, :] += part[:, :128]
        acc[1, r, :] += part[:, 128:]

    def prepare_group(g, q):
        prepare(2 * ring(jnp.where(q < 2, -g, g)) + lax.rem(q, 2))

    for g in range(1, 4):
        if g == 2:

            @pl.when(s < NS - 1)
            def _():
                pl.semaphore_wait(ready.at[0], 1)
                g_send.start()

        if g == 3:
            g_copy.wait()

            @pl.when(s > 0)
            def _():
                g_send.wait_recv()

            @pl.when(s == 0)
            def _():
                gs[6:8, :] = ini[...]

        @pl.loop(0, Q)
        def _(q):
            for d in range(2):
                b = 2 * ring(-g if d == 0 else g) + c
                ici(b, q, g - 1, d, False).wait_recv()
                ici(b, q, g, d, g == 3).start()
                d2d(b, q, g, d, False).start()
            if g == 1:
                start_group(q)
                prepare_group(1, q)
                prepare_group(2, q)
            if g == 2:
                add_group(1, q)
                prepare_group(3, q)
            if g == 3:
                add_group(2, q)

                @pl.when(q > 0)
                def _():
                    add_group(3, q - 1)

                rotate_guess(q)

    iota = lax.broadcasted_iota(jnp.int32, (8, 128), 0)
    one_v = jnp.ones((8, 128), F32)
    zero_v = jnp.zeros((8, 128), F32)
    identity = (one_v, zero_v, zero_v, one_v, zero_v, zero_v)

    def shifted(mm, k):
        return tuple(
            jnp.where(iota < k, ident, pltpu.roll(v, k, 0)) for v, ident in zip(mm, identity)
        )

    def far_arrives(q):
        b = 2 * far + c
        for d in range(2):
            ici(b, q, 3, d, True).wait_recv()
            d2d(b, q, 4, d, True).start()

    def scan_chunk(q):
        b = 2 * far + c
        r = rows(q)
        part = jnp.dot(xg[b, r, :], wi[b], preferred_element_type=F32)
        b2 = 2 * far + 1 - c
        for d in range(2):
            d2d(b2, q, 4, d, True).wait_recv()
        part += jnp.dot(xg[b2, r, :], wi[b2], preferred_element_type=F32)
        acc[0, r, :] += part[:, :128]
        acc[1, r, :] += part[:, 128:]
        mm = None
        for j in range(SEG):
            at = q * CH + j
            r1 = rot[q, j, 0]
            r2 = rot[q, j, 1]
            sq1 = jnp.tanh(r1 + acc[0, pl.ds(at, 8, stride=SEG), :])
            sq2 = jnp.tanh(r2 + acc[1, pl.ds(at, 8, stride=SEG), :])
            t1 = sq1 * sq1
            t2 = sq2 * sq2
            sl1 = 1.0 - strength * t1
            sl2 = 1.0 - strength * t2
            of1 = strength * (sq1 - r1 * (1.0 - t1))
            of2 = strength * (sq2 - r2 * (1.0 - t2))
            terms[q, j, 0] = sl1
            terms[q, j, 1] = sl2
            terms[q, j, 2] = of1
            terms[q, j, 3] = of2
            here = (sl1 * cosine, -sl1 * sine, sl2 * sine, sl2 * cosine, of1, of2)
            mm = here if mm is None else compose(here, mm)
        for k in (1, 2, 4):
            mm = compose(mm, shifted(mm, k))
        before = shifted(mm, 1)
        for i in range(6):
            seg[q, i] = before[i]
            seg[q, 6 + i] = jnp.broadcast_to(mm[i][7:8, :], (8, 128))

    @pl.loop(0, Q + 1)
    def _(q):
        @pl.when(q < Q)
        def _():
            far_arrives(q)

        @pl.when(q == 0)
        def _():
            add_group(3, Q - 1)

        @pl.when(q > 0)
        def _():
            scan_chunk(q - 1)

    def chunk_total(q):
        return tuple(seg[q, 6 + i] for i in range(6))

    whole = chunk_total(0)
    for q in range(1, Q):
        whole = compose(chunk_total(q), whole)
    for i in range(6):
        tot[i : i + 1, :] = whole[i][0:1, :]
    for i in range(6, 8):
        tot[i : i + 1, :] = jnp.zeros((1, 128), F32)

    def x_copy(dx):
        return pltpu.make_async_remote_copy(
            src_ref=tot,
            dst_ref=xbuf.at[dx],
            send_sem=x_send.at[dx],
            recv_sem=x_recv.at[dx],
            device_id=dev(zi * NX + lax.rem(xi + dx, NX), m),
            device_id_type=MESH,
        )

    @pl.when(xi < NX - 1)
    def _():
        pl.semaphore_wait(ready.at[1], NX - 1 - xi)

    for dx in range(1, NX):
        x_copy(dx).start()
    for dx in range(1, NX):
        x_copy(dx).wait_recv()

    def from_x(k):
        def member(i):
            value = whole[i]
            for dx in range(1, NX):
                here = lax.rem(xi - k + NX, NX) == dx
                value = jnp.where(here, jnp.broadcast_to(xbuf[dx, i : i + 1, :], (8, 128)), value)
            return value

        return tuple(member(i) for i in range(6))

    line = from_x(0)
    ahead = tuple(jnp.where(xi > 0, v, ident) for v, ident in zip(line, identity))
    for k in range(1, NX):
        mk = from_x(k)
        line = compose(mk, line)
        if k < NX - 1:
            more = compose(mk, ahead)
            ahead = tuple(jnp.where(xi > k, v, w) for v, w in zip(more, ahead))
    for i in range(6):
        rowtot[i : i + 1, :] = line[i][0:1, :]
    for i in range(6, 8):
        rowtot[i : i + 1, :] = jnp.zeros((1, 128), F32)

    def z_copy(dz):
        return pltpu.make_async_remote_copy(
            src_ref=rowtot,
            dst_ref=zbuf.at[dz],
            send_sem=z_send.at[dz],
            recv_sem=z_recv.at[dz],
            device_id=dev(lax.rem(zi + dz, NZ) * NX + xi, m),
            device_id_type=MESH,
        )

    @pl.when(zi < NZ - 1)
    def _():
        pl.semaphore_wait(ready.at[2], NZ - 1 - zi)

    for dz in range(1, NZ):

        @pl.when(zi + dz < NZ)
        def _():
            z_copy(dz).start()

    for dz in range(1, NZ):

        @pl.when(zi >= dz)
        def _():
            z_copy(dz).wait_recv()

    state = tuple(jnp.broadcast_to(ini[k : k + 1, :], (8, 128)) for k in range(2))
    for dz in range(NZ - 1, 0, -1):
        mk = tuple(jnp.broadcast_to(zbuf[dz, i : i + 1, :], (8, 128)) for i in range(6))
        after = apply_map(mk, state)
        state = tuple(jnp.where(zi >= dz, v, w) for v, w in zip(after, state))
    state = apply_map(ahead, state)

    entering = [state]
    for q in range(Q - 1):
        entering.append(apply_map(chunk_total(q), entering[-1]))
    current = [
        apply_map(tuple(seg[q, i] for i in range(6)), entering[q]) for q in range(Q)
    ]

    def st_copy(q, core):
        return pltpu.make_async_remote_copy(
            src_ref=stb.at[core, q],
            dst_ref=stb.at[core, q],
            send_sem=st_send.at[q],
            recv_sem=st_recv.at[q],
            device_id=partner,
            device_id_type=MESH,
        )

    for duo in ((0, 2), (1, 3)):
        states = {q: current[q] for q in duo}
        pairs = {q: ([], []) for q in duo}
        for j in range(SEG):
            for q in duo:
                x1, x2 = states[q]
                u1 = cosine * x1 - sine * x2
                u2 = sine * x1 + cosine * x2
                x1 = terms[q, j, 0] * u1 + terms[q, j, 2]
                x2 = terms[q, j, 1] * u2 + terms[q, j, 3]
                states[q] = (x1, x2)
                at = 2 * (q * CH + j)
                nsb[pl.ds(at, 8, stride=2 * SEG), :] = x1
                nsb[pl.ds(at + 1, 8, stride=2 * SEG), :] = x2
                pairs[q][0].append(x1)
                pairs[q][1].append(x2)
                if j % 2 == 1:
                    for k in range(2):
                        both = jnp.concatenate(pairs[q][k], axis=0).astype(BF16)
                        stb[c, q, (j - 1) * 8 : (j + 1) * 8, k * 128 : (k + 1) * 128] = both
                    pairs[q] = ([], [])
        for q in duo:
            st_copy(q, c).start()

    pltpu.make_async_copy(wo.at[c], wo.at[c], wo_sem.at[0]).wait()
    wo_all = pltpu.make_async_remote_copy(
        src_ref=wo.at[1 - c],
        dst_ref=wo.at[1 - c],
        send_sem=wo_sem.at[1],
        recv_sem=wo_sem.at[2],
        device_id=partner,
        device_id_type=MESH,
    )
    wo_all.wait_recv()

    def own(k, q):
        part = jnp.dot(stb[0, q], wo[0, k], preferred_element_type=F32)
        return part + jnp.dot(stb[1, q], wo[1, k], preferred_element_type=F32)

    def rs_copy(d, i):
        return pltpu.make_async_remote_copy(
            src_ref=sbuf.at[d, i],
            dst_ref=rbuf.at[d, i],
            send_sem=rs_send.at[0],
            recv_sem=rs_recv.at[d, i],
            device_id=(up, down)[d],
            device_id_type=MESH,
        )

    @pl.loop(0, 4)
    def _(i):
        for d in range(2):
            dist = (17 - i) // 4
            k = ring(dist) if d == 0 else ring(-dist)
            q = lax.rem(i + 2 * d, Q)

            @pl.when(i < 2)
            def _():
                st_copy(q, 1 - c).wait_recv()

            sbuf[d, i] = own(k, q).astype(BF16)
            rs_copy(d, i).start()

    @pl.loop(4, STEPS)
    def _(i):
        for d in range(2):
            dist = (17 - i) // 4
            k = ring(dist) if d == 0 else ring(-dist)
            q = lax.rem(i + 2 * d, Q)
            mine = own(k, q)
            rs_copy(d, i - 4).wait_recv()
            sbuf[d, i] = (mine + rbuf[d, i - 4].astype(F32)).astype(BF16)
            rs_copy(d, i).start()

    for q in (2, 0, 3, 1):
        mine = own(y, q)
        up_at = 10 + (q + 2) % 4
        down_at = 10 + q
        rs_copy(0, up_at).wait_recv()
        rs_copy(1, down_at).wait_recv()
        total = mine + rbuf[0, up_at].astype(F32) + rbuf[1, down_at].astype(F32)
        for j in range(SEG):
            for h in range(2):
                otmp[h, pl.ds(j, 8, stride=SEG), :] = total[
                    j * 8 : (j + 1) * 8, h * 128 : (h + 1) * 128
                ]
        for h in range(2):
            outb[q * CH : (q + 1) * CH, h * 128 : (h + 1) * 128] = otmp[h].astype(BF16)

    def sent(ref, sem):
        pltpu.make_async_remote_copy(
            src_ref=ref,
            dst_ref=ref,
            send_sem=sem,
            recv_sem=rs_recv.at[0, 0],
            device_id=partner,
            device_id_type=MESH,
        ).wait_send()

    sent(xg.at[pl.ds(0, 7)], ag_send.at[0])
    sent(xg.at[pl.ds(0, 8)], d2d_send.at[0])
    sent(sbuf, rs_send.at[0])
    wo_all.wait_send()

    @pl.when(s < NS - 1)
    def _():
        g_send.wait_send()

    for dx in range(1, NX):
        x_copy(dx).wait_send()
    for dz in range(1, NZ):

        @pl.when(zi + dz < NZ)
        def _():
            z_copy(dz).wait_send()

    for q in range(Q):
        st_copy(q, c).wait_send()


def local(inputs, guess, initial, w_in, bias, angle, strength, w_out):
    dma = pltpu.SemaphoreType.DMA
    hbm = pl.BlockSpec(memory_space=pltpu.HBM)
    vmem = pl.BlockSpec(memory_space=pltpu.VMEM)
    new_state, output = pl.pallas_call(
        kernel,
        out_shape=(
            jax.ShapeDtypeStruct((2 * ROWS, 128), F32),
            jax.ShapeDtypeStruct((ROWS, BLK), BF16),
        ),
        in_specs=[hbm] * 8,
        out_specs=(vmem, vmem),
        scratch_shapes=[
            pltpu.VMEM((16, ROWS, BLK), BF16),
            pltpu.VMEM((8192, 128), BF16),
            pltpu.VMEM((16, BLK, BLK), BF16),
            pltpu.VMEM((2 * BLK, 128), F32),
            pltpu.VMEM((2, NY, BLK, BLK), BF16),
            pltpu.VMEM((2, ROWS, 128), F32),
            pltpu.VMEM((8 + 2 * ROWS, 128), F32),
            pltpu.VMEM((Q, SEG, 2, 8, 128), F32),
            pltpu.VMEM((Q, SEG, 4, 8, 128), F32),
            pltpu.VMEM((Q, 12, 8, 128), F32),
            pltpu.VMEM((8, 128), F32),
            pltpu.VMEM((NX, 8, 128), F32),
            pltpu.VMEM((8, 128), F32),
            pltpu.VMEM((NZ, 8, 128), F32),
            pltpu.VMEM((2, Q, CH, BLK), BF16),
            pltpu.VMEM((2, STEPS, CH, BLK), BF16),
            pltpu.VMEM((2, STEPS, CH, BLK), BF16),
            pltpu.VMEM((2, CH, 128), F32),
            pltpu.VMEM((2, 128), F32),
            pltpu.VMEM((2, 128), F32),
            pltpu.VMEM((1, 128), F32),
            pltpu.VMEM((1, 128), F32),
            dma((7,)),
            dma((2, 4, Q)),
            dma((2, 5, Q)),
            dma((1,)),
            dma((1,)),
            dma((2,)),
            dma((3,)),
            dma((NX,)),
            dma((NX,)),
            dma((NZ,)),
            dma((NZ,)),
            dma((Q,)),
            dma((Q,)),
            dma((1,)),
            dma((2, STEPS)),
            pltpu.SemaphoreType.REGULAR((3,)),
        ],
        compiler_params=pltpu.CompilerParams(
            collective_id=0, has_side_effects=True, vmem_limit_bytes=48 * 1024 * 1024
        ),
    )(*(pltpu.with_memory_space_constraint(v, pltpu.HBM) for v in (
        inputs,
        guess.reshape(2 * ROWS, 128),
        initial,
        w_in.reshape(8192, 128),
        bias,
        angle.reshape(1, 128),
        strength.reshape(1, 128),
        w_out.reshape(BLK, 4096),
    )))
    return new_state.reshape(ROWS, 2, 128), output


def solution(mesh):
    placed = (
        P("seq", "mp"),
        P("seq", None, "mp"),
        P(None, "mp"),
        P(None, None, "mp"),
        P(None, "mp"),
        P("mp"),
        P("mp"),
        P(None, "mp", None),
    )
    return jax.shard_map(
        local,
        mesh=mesh,
        in_specs=placed,
        out_specs=(P("seq", None, "mp"), P("seq", "mp")),
        check_vma=False,
    )
```

```python
import jax
import jax.numpy as jnp
from jax import lax
from jax.experimental import pallas as pl
from jax.experimental.pallas import tpu as pltpu
from jax.sharding import PartitionSpec as P

MESH = pl.DeviceIdType.MESH
F32 = jnp.float32
BF16 = jnp.bfloat16

NY = 8
NX = 4
NZ = 8
NS = NX * NZ
ROWS = 512
BLK = 256
HALF = ROWS // 2
TALL = HALF // 2
Q = 4
CH = HALF // Q
SEG = CH // 8
STEPS = 14


def compose(later, earlier):
    a, b, c, d, e, f = later
    p, q, r, s, t, u = earlier
    return (
        a * p + b * r,
        a * q + b * s,
        c * p + d * r,
        c * q + d * s,
        a * t + b * u + e,
        c * t + d * u + f,
    )


def apply_map(m, state):
    a, b, c, d, e, f = m
    x, y = state
    return (a * x + b * y + e, c * x + d * y + f)


def kernel(
    x_hbm,
    g_hbm,
    init_hbm,
    w_hbm,
    bias_hbm,
    ang_hbm,
    str_hbm,
    wo_hbm,
    nsb,
    outb,
    xg,
    w2,
    wi,
    wtmp,
    wo,
    acc,
    gs,
    rot,
    terms,
    seg,
    xbuf,
    rowtot,
    zbuf,
    nst,
    stb,
    sbuf,
    rbuf,
    fbuf,
    pbuf,
    obuf,
    fin,
    otmp,
    ini,
    bia,
    ang,
    stg,
    loc_sem,
    small_send,
    small_recv,
    first_sem,
    ag_recv,
    far_recv,
    ag_send,
    wi_send,
    wi_recv,
    g_sem,
    e_send,
    e_recv,
    wo_sem,
    x_send,
    x_recv,
    z_send,
    z_recv,
    ns_sem,
    o_send,
    o_recv,
    rs_send,
    rs_recv,
    f_recv,
    ready,
):
    s = lax.axis_index("seq")
    m = lax.axis_index("mp")
    y = m // 2
    c = m % 2
    zi = s // NX
    xi = s % NX

    def ring(k):
        return lax.rem(y + k + 2 * NY, NY)

    def dev(seq, mp):
        return {"seq": seq, "mp": mp}

    def remote(src, dst, send, recv, target):
        return pltpu.make_async_remote_copy(
            src_ref=src,
            dst_ref=dst,
            send_sem=send,
            recv_sem=recv,
            device_id=target,
            device_id_type=MESH,
        )

    o = 1 - c
    other = 2 * y + o
    up = dev(s, ring(1) * 2 + c)
    down = dev(s, ring(-1) * 2 + c)
    partner = dev(s, other)

    barrier = pltpu.get_barrier_semaphore()

    def greet(target):
        pl.semaphore_signal(barrier, inc=1, device_id=target, device_id_type=MESH)

    greet(partner)
    for core in range(2):
        greet(dev(s, ring(1) * 2 + core))
        greet(dev(s, ring(-1) * 2 + core))

    def half_rows(core):
        return pl.ds(pl.multiple_of(core * HALF, HALF), HALF)

    in_copy = pltpu.make_async_copy(x_hbm.at[half_rows(c)], xg.at[m], loc_sem.at[0])
    in_copy.start()
    w_copy = pltpu.make_async_copy(w_hbm, w2, loc_sem.at[1])
    w_copy.start()
    small = ((init_hbm, ini), (bias_hbm, bia), (ang_hbm, ang), (str_hbm, stg))
    small_copies = [
        pltpu.make_async_copy(a, b.at[c], loc_sem.at[2 + i]) for i, (a, b) in enumerate(small)
    ]
    for copy in small_copies:
        copy.start()

    for dx in range(1, NX):

        @pl.when(xi + dx < NX)
        def _():
            for core in range(2):
                greet(dev(s + dx, 2 * y + core))

    for dz in range(1, NZ):

        @pl.when(zi + dz < NZ)
        def _():
            greet(dev(s + dz * NX, m))

    @pl.when(s < NS - 1)
    def _():
        greet(dev(s + 1, 2 * y))

    pl.semaphore_wait(barrier, 5 + 2 * xi + zi + 2 * (lax.min(s, 1) * o))

    def answer(sem, target):
        pl.semaphore_signal(sem, inc=1, device_id=target, device_id_type=MESH)

    def block_of(pos, a):
        return 2 * pos + jnp.where(a < 2, c, o)

    def tall(h):
        return pl.ds(pl.multiple_of(h * TALL, TALL), TALL)

    def ici(pos, a, g, d):
        ref = xg.at[block_of(pos, a), tall(lax.rem(a, 2))]
        return remote(ref, ref, ag_send.at[0], ag_recv.at[d, g, a], (up, down)[d])

    def far_piece(pos, slot, d):
        columns = pl.ds(d * 128, 128)
        if slot < 2:
            ref = xg.at[2 * pos + c, pl.ds(slot * TALL, TALL), columns]
        else:
            ref = xg.at[2 * pos + o, pl.ds((slot - 2) * CH, CH), columns]
        return remote(ref, ref, ag_send.at[0], far_recv.at[d, slot], (up, down)[d])

    first = remote(
        x_hbm.at[half_rows(o)], xg.at[m], first_sem.at[0], first_sem.at[1], partner
    )
    first.start()
    in_copy.wait()
    for a in range(2):
        for d in range(2):
            ici(y, a, 0, d).start()

    def small_copy(i):
        a, b = small[i]
        return remote(a, b.at[c], small_send.at[i], small_recv.at[i], partner)

    for i in range(4):
        small_copy(i).start()

    @pl.when((s > 0) & (c == 0))
    def _():
        answer(ready.at[0], dev(s - 1, 2 * y))
        answer(ready.at[0], dev(s - 1, 2 * y + 1))

    for dx in range(1, NX):

        @pl.when(xi >= dx)
        def _():
            for core in range(2):
                answer(ready.at[1], dev(s - dx, 2 * y + core))

    for dz in range(1, NZ):

        @pl.when(zi >= dz)
        def _():
            answer(ready.at[2], dev(s - dz * NX, m))

    def guess_own(core):
        if core == 0:
            return pltpu.make_async_copy(
                g_hbm.at[pl.ds(0, 2 * HALF)], gs.at[0, pl.ds(8, 2 * HALF)], loc_sem.at[6]
            )
        return pltpu.make_async_copy(
            g_hbm.at[pl.ds(2 * HALF - 8, 2 * HALF + 8)], gs.at[1], loc_sem.at[6]
        )

    def guess_to(core):
        pb = 1 - core
        if core == 0:
            return remote(
                g_hbm.at[pl.ds(0, 2 * HALF)],
                gs.at[pb, pl.ds(8, 2 * HALF)],
                g_sem.at[0],
                g_sem.at[1],
                partner,
            )
        return remote(
            g_hbm.at[pl.ds(2 * HALF - 8, 2 * HALF + 8)],
            gs.at[pb],
            g_sem.at[0],
            g_sem.at[1],
            partner,
        )

    first_recv = first.wait_recv
    w_copy.wait()

    def prepare(b):
        wtmp[...] = w2[pl.ds(pl.multiple_of(b * 2 * BLK, 2 * BLK), 2 * BLK), :].astype(F32)
        for k in range(2):
            wi[c, b, :, k * 128 : (k + 1) * 128] = wtmp[pl.ds(k, BLK, stride=2), :].astype(BF16)
        wi_copy(c, b).start()

    def wi_copy(pb, b):
        return remote(wi.at[pb, b], wi.at[pb, b], wi_send.at[0], wi_recv.at[b], partner)

    prepare(m)
    first_recv()
    for a in range(2, 4):
        for d in range(2):
            ici(y, a, 0, d).start()
    prepare(other)

    for core in range(2):

        @pl.when(c == core)
        def _():
            guess_own(core).start()
            guess_to(1 - core).start()

    far = ring(4)
    prepare(2 * far)
    prepare(2 * far + 1)

    for copy in small_copies:
        copy.wait()
    for i in range(4):
        small_copy(i).wait_recv()

    def lanes(v):
        return jnp.broadcast_to(v, (8, 128))

    cosine = [lanes(jnp.cos(ang[pb])) for pb in range(2)]
    sine = [lanes(jnp.sin(ang[pb])) for pb in range(2)]
    strength = [lanes(stg[pb]) for pb in range(2)]

    def products(b, r):
        lhs = xg[b, r, :]
        return [jnp.dot(lhs, wi[pb, b], preferred_element_type=F32) for pb in range(2)]

    def start_group(h):
        r = tall(h)

        @pl.when(h == 0)
        def _():
            wi_copy(o, m).wait_recv()
            wi_copy(o, other).wait_recv()

        one = products(m, r)
        two = products(other, r)
        for pb in range(2):
            part = one[pb] + two[pb]
            acc[2 * pb, r, :] = part[:, :128] + bia[pb, 0:1, :]
            acc[2 * pb + 1, r, :] = part[:, 128:] + bia[pb, 1:2, :]

    def add_blocks(blocks, r):
        part = None
        for b in blocks:
            term = products(b, r)
            part = term if part is None else [u + v for u, v in zip(part, term)]
        for pb in range(2):
            acc[2 * pb, r, :] += part[pb][:, :128]
            acc[2 * pb + 1, r, :] += part[pb][:, 128:]

    def add_group(g, h):
        blocks = [2 * ring(k) + core for k in (-g, g) for core in range(2)]

        def weights():
            for b in blocks:
                wi_copy(o, b).wait_recv()

        if isinstance(h, int):
            if h == 0:
                weights()
            add_blocks(blocks, pl.ds(h * TALL, TALL))
        else:
            pl.when(h == 0)(weights)
            add_blocks(blocks, tall(h))

    def rotate_guess(q):
        @pl.loop(0, SEG)
        def _(j):
            at = 6 + 2 * (q * CH + j)
            for pb in range(2):
                one = gs[pb, pl.ds(at, 8, stride=2 * SEG), :]
                two = gs[pb, pl.ds(at + 1, 8, stride=2 * SEG), :]
                rot[q, j, 2 * pb] = cosine[pb] * one - sine[pb] * two
                rot[q, j, 2 * pb + 1] = sine[pb] * one + cosine[pb] * two

    def prepare_group(g, i):
        prepare(2 * ring(jnp.where(i < 2, -g, g)) + lax.rem(i, 2))

    def edge(pb):
        return remote(
            g_hbm.at[pl.ds(2 * ROWS - 8, 8)],
            gs.at[pb, pl.ds(0, 8)],
            e_send.at[0],
            e_recv.at[pb],
            dev(lax.rem(s + 1, NS), 2 * y),
        )

    def wo_cols(k):
        return wo_hbm.at[:, pl.ds(k * BLK, BLK)]

    def wo_copy(k):
        return remote(wo_cols(k), wo.at[c, k], wo_sem.at[1], wo_sem.at[2], partner)

    for g in range(1, 4):
        if g == 2:
            for k in range(2 * NY):
                pltpu.make_async_copy(wo_cols(k), wo.at[c, k], wo_sem.at[0]).start()
                wo_copy(k).start()

            @pl.when(s < NS - 1)
            def _():
                pl.semaphore_wait(ready.at[0], 1)
                edge(c).start()

        if g == 3:
            for core in range(2):

                @pl.when(c == core)
                def _():
                    guess_own(core).wait()
                    guess_to(core).wait_recv()

            @pl.when((s > 0) & (c == 0))
            def _():
                for pb in range(2):
                    edge(pb).wait_recv()

            @pl.when((s == 0) & (c == 0))
            def _():
                for pb in range(2):
                    gs[pb, 6:8, :] = ini[pb]

            for a in range(4):
                for d in range(2):
                    pos = ring(-3 if d == 0 else 3)
                    ici(pos, a, 2, d).wait_recv()
                    for slot in ((0,), (1,), (2, 3), (4, 5))[a]:
                        far_piece(pos, slot, d).start()
                if a < 2:
                    add_group(2, a)
                if a == 3:
                    add_group(3, 0)
                rotate_guess(a)
        else:

            @pl.loop(0, 4)
            def _(a):
                for d in range(2):
                    pos = ring(-g if d == 0 else g)
                    ici(pos, a, g - 1, d).wait_recv()
                    ici(pos, a, g, d).start()
                if g == 1:
                    prepare_group(1, a)
                    prepare_group(2, a)
                else:
                    prepare_group(3, a)

                @pl.when(lax.rem(a, 2) == 1)
                def _():
                    if g == 1:
                        start_group(a // 2)
                    else:
                        add_group(1, a // 2)

    iota = lax.broadcasted_iota(jnp.int32, (8, 128), 0)
    one_v = jnp.ones((8, 128), F32)
    zero_v = jnp.zeros((8, 128), F32)
    identity = (one_v, zero_v, zero_v, one_v, zero_v, zero_v)

    def shifted(mm, k):
        return tuple(
            jnp.where(iota < k, ident, pltpu.roll(v, k, 0)) for v, ident in zip(mm, identity)
        )

    def scan_chunk(q):
        for d in range(2):
            for slot in ((0, 2), (3,), (1, 4), (5,))[q]:
                far_piece(far, slot, d).wait_recv()
        if q == 0:
            add_group(3, 1)
            wi_copy(o, 2 * far).wait_recv()
            wi_copy(o, 2 * far + 1).wait_recv()
        add_blocks((2 * far, 2 * far + 1), pl.ds(q * CH, CH))
        mm = [None, None]
        for j in range(SEG):
            at = q * CH + j
            for pb in range(2):
                st = strength[pb]
                r1 = rot[q, j, 2 * pb]
                r2 = rot[q, j, 2 * pb + 1]
                sq1 = jnp.tanh(r1 + acc[2 * pb, pl.ds(at, 8, stride=SEG), :])
                sq2 = jnp.tanh(r2 + acc[2 * pb + 1, pl.ds(at, 8, stride=SEG), :])
                t1 = sq1 * sq1
                t2 = sq2 * sq2
                sl1 = 1.0 - st * t1
                sl2 = 1.0 - st * t2
                of1 = st * (sq1 - r1 * (1.0 - t1))
                of2 = st * (sq2 - r2 * (1.0 - t2))
                for i, v in enumerate((sl1, sl2, of1, of2)):
                    terms[q, j, 4 * pb + i] = v
                co, si = cosine[pb], sine[pb]
                here = (sl1 * co, -sl1 * si, sl2 * si, sl2 * co, of1, of2)
                mm[pb] = here if mm[pb] is None else compose(here, mm[pb])
        for k in (1, 2, 4):
            mm = [compose(v, shifted(v, k)) for v in mm]
        for pb in range(2):
            before = shifted(mm[pb], 1)
            for i in range(6):
                seg[q, pb, i] = before[i]
                seg[q, pb, 6 + i] = lanes(mm[pb][i][7:8, :])

    for q in range(Q):
        scan_chunk(q)

    def chunk_total(q, pb):
        return tuple(seg[q, pb, 6 + i] for i in range(6))

    place = 2 * xi + c
    for pb in range(2):
        whole = chunk_total(0, pb)
        for q in range(1, Q):
            whole = compose(chunk_total(q, pb), whole)
        for i in range(6):
            xbuf[place, 6 * pb + i : 6 * pb + i + 1, :] = whole[i][0:1, :]

    def x_copy(dx, core):
        ref = xbuf.at[place]
        target = dev(zi * NX + lax.rem(xi + dx, NX), 2 * y + core)
        return remote(ref, ref, x_send.at[dx, core], x_recv.at[place], target)

    def x_arrival(k):
        return remote(xbuf.at[k], xbuf.at[k], x_send.at[0, 0], x_recv.at[k], partner)

    def to_line(act):
        act(remote(xbuf.at[place], xbuf.at[place], x_send.at[0, 0], x_recv.at[place], partner))
        for dx in range(1, NX):
            for core in range(2):
                act(x_copy(dx, core))

    @pl.when(xi < NX - 1)
    def _():
        pl.semaphore_wait(ready.at[1], 2 * (NX - 1 - xi))

    to_line(lambda copy: copy.start())
    for k in range(2 * NX):

        @pl.when(place != k)
        def _():
            x_arrival(k).wait_recv()

    def member(k, pb):
        return tuple(lanes(xbuf[k, 6 * pb + i : 6 * pb + i + 1, :]) for i in range(6))

    partial = [[member(0, pb)] for pb in range(2)]
    for k in range(1, 2 * NX):
        for pb in range(2):
            partial[pb].append(compose(member(k, pb), partial[pb][-1]))
    for pb in range(2):
        for i in range(6):
            rowtot[6 * pb + i : 6 * pb + i + 1, :] = partial[pb][-1][i][0:1, :]

    def z_copy(dz):
        target = dev(lax.rem(zi + dz, NZ) * NX + xi, m)
        return remote(rowtot, zbuf.at[dz], z_send.at[dz], z_recv.at[dz], target)

    @pl.when(zi < NZ - 1)
    def _():
        pl.semaphore_wait(ready.at[2], NZ - 1 - zi)

    for dz in range(1, NZ):

        @pl.when(zi + dz < NZ)
        def _():
            z_copy(dz).start()

    ahead = []
    for pb in range(2):
        before = identity
        for k in range(2 * NX - 1):
            before = tuple(
                jnp.where(place == k + 1, v, w) for v, w in zip(partial[pb][k], before)
            )
        ahead.append(before)

    for dz in range(1, NZ):

        @pl.when(zi >= dz)
        def _():
            z_copy(dz).wait_recv()

    current = {}
    for pb in range(2):
        state = tuple(lanes(ini[pb, k : k + 1, :]) for k in range(2))
        for dz in range(NZ - 1, 0, -1):
            mk = tuple(lanes(zbuf[dz, 6 * pb + i : 6 * pb + i + 1, :]) for i in range(6))
            after = apply_map(mk, state)
            state = tuple(jnp.where(zi >= dz, v, w) for v, w in zip(after, state))
        state = apply_map(ahead[pb], state)
        for q in range(Q):
            current[q, pb] = apply_map(tuple(seg[q, pb, i] for i in range(6)), state)
            if q < Q - 1:
                state = apply_map(chunk_total(q, pb), state)

    for duo in ((0, 1), (2, 3)):
        chains = [(q, pb) for q in duo for pb in range(2)]
        pairs = {chain: ([], []) for chain in chains}
        for j in range(SEG):
            for q, pb in chains:
                x1, x2 = current[q, pb]
                u1 = cosine[pb] * x1 - sine[pb] * x2
                u2 = sine[pb] * x1 + cosine[pb] * x2
                x1 = terms[q, j, 4 * pb] * u1 + terms[q, j, 4 * pb + 2]
                x2 = terms[q, j, 4 * pb + 1] * u2 + terms[q, j, 4 * pb + 3]
                current[q, pb] = (x1, x2)
                at = 2 * (q * CH + j)
                nst[pb, pl.ds(at, 8, stride=2 * SEG), :] = x1
                nst[pb, pl.ds(at + 1, 8, stride=2 * SEG), :] = x2
                pairs[q, pb][0].append(x1)
                pairs[q, pb][1].append(x2)
                if j % 2 == 1:
                    for k in range(2):
                        both = jnp.concatenate(pairs[q, pb][k], axis=0).astype(BF16)
                        top = (q % 2) * CH + (j - 1) * 8
                        stb[pb, q // 2, top : top + 16, k * 128 : (k + 1) * 128] = both
                    pairs[q, pb] = ([], [])

    pltpu.make_async_copy(wo.at[c], wo.at[c], wo_sem.at[0]).wait()
    wo_all = remote(wo.at[o], wo.at[o], wo_sem.at[1], wo_sem.at[2], partner)
    wo_all.wait_recv()

    def own(k, q):
        columns = 2 * k + q // 2
        h = lax.rem(q, 2)
        part = jnp.dot(stb[0, h], wo[0, columns], preferred_element_type=F32)
        return part + jnp.dot(stb[1, h], wo[1, columns], preferred_element_type=F32)

    def rs_copy(d, i):
        return remote(
            sbuf.at[d, i], rbuf.at[d, i], rs_send.at[0], rs_recv.at[d, i], (up, down)[d]
        )

    def last_copy(d, i):
        q = lax.rem(i + 2 * d, 4)
        h = lax.rem(q, 2)
        target = dev(s, 2 * ring(1 if d == 0 else -1) + q // 2)
        return remote(
            sbuf.at[d, i], fbuf.at[d, c, h], rs_send.at[0], f_recv.at[d, c, h], target
        )

    def item(d, i):
        dist = (17 - i) // 4
        return own(ring(dist) if d == 0 else ring(-dist), lax.rem(i + 2 * d, 4))

    @pl.loop(0, 4)
    def _(i):
        for d in range(2):
            sbuf[d, i] = item(d, i).astype(BF16)
            rs_copy(d, i).start()

    def home(h):
        ref = nsb.at[pl.ds(pl.multiple_of(c * 2 * HALF, 2 * HALF), 2 * HALF)]
        if h == 0:
            return pltpu.make_async_copy(nst.at[c], ref, ns_sem.at[0])
        return remote(nst.at[o], ref, ns_sem.at[1], ns_sem.at[2], partner)

    home(0).start()
    home(1).start()

    def own_copy(h):
        return remote(pbuf.at[h], obuf.at[h], o_send.at[h], o_recv.at[h], partner)

    @pl.loop(4, 10)
    def _(i):
        for d in range(2):
            mine = item(d, i)
            rs_copy(d, i - 4).wait_recv()
            sbuf[d, i] = (mine + rbuf[d, i - 4].astype(F32)).astype(BF16)
            rs_copy(d, i).start()

        @pl.when(i < 6)
        def _():
            h = i - 4
            fin[h] = own(y, 2 * c + h)
            pbuf[h] = own(y, 2 * o + h).astype(BF16)
            own_copy(h).start()

    @pl.loop(10, STEPS)
    def _(i):
        for d in range(2):
            mine = item(d, i)
            rs_copy(d, i - 4).wait_recv()
            sbuf[d, i] = (mine + rbuf[d, i - 4].astype(F32)).astype(BF16)
            last_copy(d, i).start()

    def landed(d, core, h):
        ref = fbuf.at[d, core, h]
        return remote(ref, ref, rs_send.at[0], f_recv.at[d, core, h], partner)

    for h in range(2):
        own_copy(h).wait_recv()
        for mine in (True, False):
            core = c if mine else o
            base = fin[h] if mine else obuf[h].astype(F32)
            landed(o, core, h).wait_recv()
            fin[h if mine else 2 + h] = base + fbuf[o, core, h].astype(F32)
    for h in range(2):
        for mine in (True, False):
            core = c if mine else o
            landed(c, core, h).wait_recv()
            total = fin[h if mine else 2 + h] + fbuf[c, core, h].astype(F32)
            slot = 0 if mine else 1
            for u in range(TALL // CH):
                for j in range(SEG):
                    for k in range(2):
                        top = u * CH + j * 8
                        otmp[slot, k, pl.ds(u * CH + j, 8, stride=SEG), :] = total[
                            top : top + 8, k * 128 : (k + 1) * 128
                        ]
            r = pl.ds(pl.multiple_of(core * HALF + h * TALL, TALL), TALL)
            for k in range(2):
                outb[r, k * 128 : (k + 1) * 128] = otmp[slot, k].astype(BF16)

    def sent(ref, sem):
        remote(ref, ref, sem, rs_recv.at[0, 0], partner).wait_send()

    first.wait_send()
    for i in range(4):
        small_copy(i).wait_send()
    for core in range(2):

        @pl.when(c == core)
        def _():
            guess_to(1 - core).wait_send()

    @pl.when(s < NS - 1)
    def _():
        edge(c).wait_send()

    sent(xg.at[pl.ds(0, 14)], ag_send.at[0])
    sent(wi.at[c], wi_send.at[0])
    wo_all.wait_send()
    to_line(lambda copy: copy.wait_send())
    for dz in range(1, NZ):

        @pl.when(zi + dz < NZ)
        def _():
            z_copy(dz).wait_send()

    home(0).wait()
    home(1).wait_send()
    other_half = nsb.at[pl.ds(pl.multiple_of(o * 2 * HALF, 2 * HALF), 2 * HALF)]
    remote(nst.at[o], other_half, ns_sem.at[1], ns_sem.at[2], partner).wait_recv()
    for h in range(2):
        own_copy(h).wait_send()
    sent(sbuf, rs_send.at[0])


def write_out(state, out, state_hbm, out_hbm, sem):
    copies = (
        pltpu.make_async_copy(state, state_hbm, sem.at[0]),
        pltpu.make_async_copy(out, out_hbm, sem.at[1]),
    )
    for copy in copies:
        copy.start()
    for copy in copies:
        copy.wait()


def local(inputs, guess, initial, w_in, bias, angle, strength, w_out):
    dma = pltpu.SemaphoreType.DMA
    hbm = pl.BlockSpec(memory_space=pltpu.HBM)
    vmem = pl.BlockSpec(memory_space=pltpu.VMEM)
    new_state, output = pl.pallas_call(
        kernel,
        out_shape=(
            jax.ShapeDtypeStruct((2 * ROWS, 128), F32),
            jax.ShapeDtypeStruct((ROWS, BLK), BF16),
        ),
        in_specs=[hbm] * 8,
        out_specs=(vmem, vmem),
        scratch_shapes=[
            pltpu.VMEM((16, HALF, BLK), BF16),
            pltpu.VMEM((8192, 128), BF16),
            pltpu.VMEM((2, 16, BLK, BLK), BF16),
            pltpu.VMEM((2 * BLK, 128), F32),
            pltpu.VMEM((2, 16, BLK, BLK), BF16),
            pltpu.VMEM((4, HALF, 128), F32),
            pltpu.VMEM((2, 8 + 2 * HALF, 128), F32),
            pltpu.VMEM((Q, SEG, 4, 8, 128), F32),
            pltpu.VMEM((Q, SEG, 8, 8, 128), F32),
            pltpu.VMEM((Q, 2, 12, 8, 128), F32),
            pltpu.VMEM((2 * NX, 12, 128), F32),
            pltpu.VMEM((12, 128), F32),
            pltpu.VMEM((NZ, 12, 128), F32),
            pltpu.VMEM((2, 2 * HALF, 128), F32),
            pltpu.VMEM((2, 2, TALL, BLK), BF16),
            pltpu.VMEM((2, STEPS, TALL, BLK), BF16),
            pltpu.VMEM((2, 10, TALL, BLK), BF16),
            pltpu.VMEM((2, 2, 2, TALL, BLK), BF16),
            pltpu.VMEM((2, TALL, BLK), BF16),
            pltpu.VMEM((2, TALL, BLK), BF16),
            pltpu.VMEM((4, TALL, BLK), F32),
            pltpu.VMEM((2, 2, TALL, 128), F32),
            pltpu.VMEM((2, 2, 128), F32),
            pltpu.VMEM((2, 2, 128), F32),
            pltpu.VMEM((2, 1, 128), F32),
            pltpu.VMEM((2, 1, 128), F32),
            dma((7,)),
            dma((4,)),
            dma((4,)),
            dma((2,)),
            dma((2, 3, 4)),
            dma((2, 6)),
            dma((1,)),
            dma((1,)),
            dma((16,)),
            dma((2,)),
            dma((1,)),
            dma((2,)),
            dma((3,)),
            dma((NX, 2)),
            dma((2 * NX,)),
            dma((NZ,)),
            dma((NZ,)),
            dma((3,)),
            dma((2,)),
            dma((2,)),
            dma((1,)),
            dma((2, 10)),
            dma((2, 2, 2)),
            pltpu.SemaphoreType.REGULAR((3,)),
        ],
        compiler_params=pltpu.CompilerParams(
            collective_id=0, has_side_effects=True, vmem_limit_bytes=48 * 1024 * 1024
        ),
    )(*(pltpu.with_memory_space_constraint(v, pltpu.HBM) for v in (
        inputs,
        guess.reshape(2 * ROWS, 128),
        initial,
        w_in.reshape(8192, 128),
        bias,
        angle.reshape(1, 128),
        strength.reshape(1, 128),
        w_out.reshape(BLK, 4096),
    )))
    new_state, output = pl.pallas_call(
        write_out,
        out_shape=(
            jax.ShapeDtypeStruct((2 * ROWS, 128), F32),
            jax.ShapeDtypeStruct((ROWS, BLK), BF16),
        ),
        in_specs=[pl.BlockSpec(memory_space=pl.ANY)] * 2,
        out_specs=(hbm, hbm),
        scratch_shapes=[dma((2,))],
        compiler_params=pltpu.CompilerParams(vmem_limit_bytes=4 * 1024 * 1024),
    )(new_state, output)
    return new_state.reshape(ROWS, 2, 128), output


def solution(mesh):
    placed = (
        P("seq", "mp"),
        P("seq", None, "mp"),
        P(None, "mp"),
        P(None, None, "mp"),
        P(None, "mp"),
        P("mp"),
        P("mp"),
        P(None, "mp", None),
    )
    return jax.shard_map(
        local,
        mesh=mesh,
        in_specs=placed,
        out_specs=(P("seq", None, "mp"), P("seq", "mp")),
        check_vma=False,
    )
```

```python
import jax
import jax.numpy as jnp
from jax import lax
from jax.experimental import pallas as pl
from jax.experimental.pallas import tpu as pltpu
from jax.sharding import PartitionSpec as P

MESH = pl.DeviceIdType.MESH
F32 = jnp.float32
BF16 = jnp.bfloat16

NY = 8
NX = 4
NZ = 8
NS = NX * NZ
ROWS = 512
BLK = 256
HALF = ROWS // 2
TALL = HALF // 2
Q = 4
CH = HALF // Q
SEG = CH // 8
LEAD = 1
STEPS = 14


def compose(later, earlier):
    a, b, c, d, e, f = later
    p, q, r, s, t, u = earlier
    return (
        a * p + b * r,
        a * q + b * s,
        c * p + d * r,
        c * q + d * s,
        a * t + b * u + e,
        c * t + d * u + f,
    )


def apply_map(m, state):
    a, b, c, d, e, f = m
    x, y = state
    return (a * x + b * y + e, c * x + d * y + f)


def kernel(
    x_hbm,
    g_hbm,
    init_hbm,
    w_hbm,
    bias_hbm,
    ang_hbm,
    str_hbm,
    wo_hbm,
    nsb,
    outb,
    xg,
    w2,
    wi,
    wtmp,
    wo,
    acc,
    gs,
    rot,
    terms,
    seg,
    hbuf,
    ebuf,
    xbuf,
    rowtot,
    zbuf,
    nst,
    stb,
    sbuf,
    rbuf,
    fbuf,
    pbuf,
    obuf,
    fin,
    otmp,
    ini,
    bia,
    ang,
    stg,
    loc_sem,
    small_send,
    small_recv,
    first_sem,
    ag_recv,
    far_recv,
    ag_send,
    wi_send,
    wi_recv,
    g_sem,
    e_send,
    e_recv,
    wo_sem,
    h_sem,
    x_send,
    x_recv,
    z_send,
    z_recv,
    ns_sem,
    o_send,
    o_recv,
    rs_send,
    rs_recv,
    f_recv,
    ready,
):
    s = lax.axis_index("seq")
    m = lax.axis_index("mp")
    y = m // 2
    c = m % 2
    zi = s // NX
    xi = s % NX

    def ring(k):
        return lax.rem(y + k + 2 * NY, NY)

    def dev(seq, mp):
        return {"seq": seq, "mp": mp}

    def remote(src, dst, send, recv, target):
        return pltpu.make_async_remote_copy(
            src_ref=src,
            dst_ref=dst,
            send_sem=send,
            recv_sem=recv,
            device_id=target,
            device_id_type=MESH,
        )

    o = 1 - c
    other = 2 * y + o
    up = dev(s, ring(1) * 2 + c)
    down = dev(s, ring(-1) * 2 + c)
    partner = dev(s, other)

    barrier = pltpu.get_barrier_semaphore()

    def greet(target):
        pl.semaphore_signal(barrier, inc=1, device_id=target, device_id_type=MESH)

    greet(partner)
    for core in range(2):
        greet(dev(s, ring(1) * 2 + core))
        greet(dev(s, ring(-1) * 2 + core))

    def half_rows(core):
        return pl.ds(pl.multiple_of(core * HALF, HALF), HALF)

    in_copy = pltpu.make_async_copy(x_hbm.at[half_rows(c)], xg.at[m], loc_sem.at[0])
    in_copy.start()
    w_copy = pltpu.make_async_copy(w_hbm, w2, loc_sem.at[1])
    w_copy.start()
    small = ((init_hbm, ini), (bias_hbm, bia), (ang_hbm, ang), (str_hbm, stg))
    small_copies = [
        pltpu.make_async_copy(a, b.at[c], loc_sem.at[2 + i]) for i, (a, b) in enumerate(small)
    ]
    for copy in small_copies:
        copy.start()

    for dx in range(1, NX):

        @pl.when((xi + dx < NX) & (c == LEAD))
        def _():
            greet(dev(s + dx, m))

    for dz in range(1, NZ):

        @pl.when((zi + dz < NZ) & (c == LEAD))
        def _():
            greet(dev(s + dz * NX, m))

    @pl.when(s < NS - 1)
    def _():
        greet(dev(s + 1, 2 * y))

    pl.semaphore_wait(barrier, 5 + (c if LEAD == 1 else o) * (xi + zi) + 2 * (lax.min(s, 1) * o))

    def answer(sem, target):
        pl.semaphore_signal(sem, inc=1, device_id=target, device_id_type=MESH)

    def block_of(pos, a):
        return 2 * pos + jnp.where(a < 2, c, o)

    def tall(h):
        return pl.ds(pl.multiple_of(h * TALL, TALL), TALL)

    def ici(pos, a, g, d):
        ref = xg.at[block_of(pos, a), tall(lax.rem(a, 2))]
        return remote(ref, ref, ag_send.at[0], ag_recv.at[d, g, a], (up, down)[d])

    def far_piece(pos, slot, d):
        columns = pl.ds(d * 128, 128)
        if slot < 2:
            ref = xg.at[2 * pos + c, pl.ds(slot * TALL, TALL), columns]
        else:
            ref = xg.at[2 * pos + o, pl.ds((slot - 2) * CH, CH), columns]
        return remote(ref, ref, ag_send.at[0], far_recv.at[d, slot], (up, down)[d])

    first = remote(
        x_hbm.at[half_rows(o)], xg.at[m], first_sem.at[0], first_sem.at[1], partner
    )
    first.start()
    in_copy.wait()
    for a in range(2):
        for d in range(2):
            ici(y, a, 0, d).start()

    def small_copy(i):
        a, b = small[i]
        return remote(a, b.at[c], small_send.at[i], small_recv.at[i], partner)

    for i in range(4):
        small_copy(i).start()

    @pl.when((s > 0) & (c == 0))
    def _():
        answer(ready.at[0], dev(s - 1, 2 * y))
        answer(ready.at[0], dev(s - 1, 2 * y + 1))

    for dx in range(1, NX):

        @pl.when((xi >= dx) & (c == LEAD))
        def _():
            answer(ready.at[1], dev(s - dx, m))

    for dz in range(1, NZ):

        @pl.when((zi >= dz) & (c == LEAD))
        def _():
            answer(ready.at[2], dev(s - dz * NX, m))

    def guess_own(core):
        if core == 0:
            return pltpu.make_async_copy(
                g_hbm.at[pl.ds(0, 2 * HALF)], gs.at[0, pl.ds(8, 2 * HALF)], loc_sem.at[6]
            )
        return pltpu.make_async_copy(
            g_hbm.at[pl.ds(2 * HALF - 8, 2 * HALF + 8)], gs.at[1], loc_sem.at[6]
        )

    def guess_to(core):
        pb = 1 - core
        if core == 0:
            return remote(
                g_hbm.at[pl.ds(0, 2 * HALF)],
                gs.at[pb, pl.ds(8, 2 * HALF)],
                g_sem.at[0],
                g_sem.at[1],
                partner,
            )
        return remote(
            g_hbm.at[pl.ds(2 * HALF - 8, 2 * HALF + 8)],
            gs.at[pb],
            g_sem.at[0],
            g_sem.at[1],
            partner,
        )

    first_recv = first.wait_recv
    w_copy.wait()

    def prepare(b):
        wtmp[...] = w2[pl.ds(pl.multiple_of(b * 2 * BLK, 2 * BLK), 2 * BLK), :].astype(F32)
        for k in range(2):
            wi[c, b, :, k * 128 : (k + 1) * 128] = wtmp[pl.ds(k, BLK, stride=2), :].astype(BF16)
        wi_copy(c, b).start()

    def wi_copy(pb, b):
        return remote(wi.at[pb, b], wi.at[pb, b], wi_send.at[0], wi_recv.at[b], partner)

    prepare(m)
    first_recv()
    for a in range(2, 4):
        for d in range(2):
            ici(y, a, 0, d).start()
    prepare(other)

    for core in range(2):

        @pl.when(c == core)
        def _():
            guess_own(core).start()
            guess_to(1 - core).start()

    far = ring(4)
    prepare(2 * far)
    prepare(2 * far + 1)

    for copy in small_copies:
        copy.wait()
    for i in range(4):
        small_copy(i).wait_recv()

    def lanes(v):
        return jnp.broadcast_to(v, (8, 128))

    cosine = [lanes(jnp.cos(ang[pb])) for pb in range(2)]
    sine = [lanes(jnp.sin(ang[pb])) for pb in range(2)]
    strength = [lanes(stg[pb]) for pb in range(2)]

    def products(b, r):
        lhs = xg[b, r, :]
        return [jnp.dot(lhs, wi[pb, b], preferred_element_type=F32) for pb in range(2)]

    def start_group(h):
        r = tall(h)

        @pl.when(h == 0)
        def _():
            wi_copy(o, m).wait_recv()
            wi_copy(o, other).wait_recv()

        one = products(m, r)
        two = products(other, r)
        for pb in range(2):
            part = one[pb] + two[pb]
            acc[2 * pb, r, :] = part[:, :128] + bia[pb, 0:1, :]
            acc[2 * pb + 1, r, :] = part[:, 128:] + bia[pb, 1:2, :]

    def add_blocks(blocks, r):
        part = None
        for b in blocks:
            term = products(b, r)
            part = term if part is None else [u + v for u, v in zip(part, term)]
        for pb in range(2):
            acc[2 * pb, r, :] += part[pb][:, :128]
            acc[2 * pb + 1, r, :] += part[pb][:, 128:]

    def add_group(g, h):
        blocks = [2 * ring(k) + core for k in (-g, g) for core in range(2)]

        def weights():
            for b in blocks:
                wi_copy(o, b).wait_recv()

        if isinstance(h, int):
            if h == 0:
                weights()
            add_blocks(blocks, pl.ds(h * TALL, TALL))
        else:
            pl.when(h == 0)(weights)
            add_blocks(blocks, tall(h))

    def rotate_guess(q):
        @pl.loop(0, SEG)
        def _(j):
            at = 6 + 2 * (q * CH + j)
            for pb in range(2):
                one = gs[pb, pl.ds(at, 8, stride=2 * SEG), :]
                two = gs[pb, pl.ds(at + 1, 8, stride=2 * SEG), :]
                rot[q, j, 2 * pb] = cosine[pb] * one - sine[pb] * two
                rot[q, j, 2 * pb + 1] = sine[pb] * one + cosine[pb] * two

    def prepare_group(g, i):
        prepare(2 * ring(jnp.where(i < 2, -g, g)) + lax.rem(i, 2))

    def edge(pb):
        return remote(
            g_hbm.at[pl.ds(2 * ROWS - 8, 8)],
            gs.at[pb, pl.ds(0, 8)],
            e_send.at[0],
            e_recv.at[pb],
            dev(lax.rem(s + 1, NS), 2 * y),
        )

    def wo_cols(k):
        return wo_hbm.at[:, pl.ds(k * BLK, BLK)]

    def wo_copy(k):
        return remote(wo_cols(k), wo.at[c, k], wo_sem.at[1], wo_sem.at[2], partner)

    for g in range(1, 4):
        if g == 2:
            for k in range(2 * NY):
                pltpu.make_async_copy(wo_cols(k), wo.at[c, k], wo_sem.at[0]).start()
                wo_copy(k).start()

            @pl.when(s < NS - 1)
            def _():
                pl.semaphore_wait(ready.at[0], 1)
                edge(c).start()

        if g == 3:
            for core in range(2):

                @pl.when(c == core)
                def _():
                    guess_own(core).wait()
                    guess_to(core).wait_recv()

            @pl.when((s > 0) & (c == 0))
            def _():
                for pb in range(2):
                    edge(pb).wait_recv()

            @pl.when((s == 0) & (c == 0))
            def _():
                for pb in range(2):
                    gs[pb, 6:8, :] = ini[pb]

            for a in range(4):
                for d in range(2):
                    pos = ring(-3 if d == 0 else 3)
                    ici(pos, a, 2, d).wait_recv()
                    for slot in ((0,), (1,), (2, 3), (4, 5))[a]:
                        far_piece(pos, slot, d).start()
                if a < 2:
                    add_group(2, a)
                if a == 3:
                    add_group(3, 0)
                rotate_guess(a)
        else:

            @pl.loop(0, 4)
            def _(a):
                for d in range(2):
                    pos = ring(-g if d == 0 else g)
                    ici(pos, a, g - 1, d).wait_recv()
                    ici(pos, a, g, d).start()
                if g == 1:
                    prepare_group(1, a)
                    prepare_group(2, a)
                else:
                    prepare_group(3, a)

                @pl.when(lax.rem(a, 2) == 1)
                def _():
                    if g == 1:
                        start_group(a // 2)
                    else:
                        add_group(1, a // 2)

    iota = lax.broadcasted_iota(jnp.int32, (8, 128), 0)
    one_v = jnp.ones((8, 128), F32)
    zero_v = jnp.zeros((8, 128), F32)
    identity = (one_v, zero_v, zero_v, one_v, zero_v, zero_v)

    def shifted(mm, k):
        return tuple(
            jnp.where(iota < k, ident, pltpu.roll(v, k, 0)) for v, ident in zip(mm, identity)
        )

    def scan_chunk(q):
        for d in range(2):
            for slot in ((0, 2), (3,), (1, 4), (5,))[q]:
                far_piece(far, slot, d).wait_recv()
        if q == 0:
            add_group(3, 1)
            wi_copy(o, 2 * far).wait_recv()
            wi_copy(o, 2 * far + 1).wait_recv()
        add_blocks((2 * far, 2 * far + 1), pl.ds(q * CH, CH))
        mm = [None, None]
        for j in range(SEG):
            at = q * CH + j
            for pb in range(2):
                st = strength[pb]
                r1 = rot[q, j, 2 * pb]
                r2 = rot[q, j, 2 * pb + 1]
                sq1 = jnp.tanh(r1 + acc[2 * pb, pl.ds(at, 8, stride=SEG), :])
                sq2 = jnp.tanh(r2 + acc[2 * pb + 1, pl.ds(at, 8, stride=SEG), :])
                t1 = sq1 * sq1
                t2 = sq2 * sq2
                sl1 = 1.0 - st * t1
                sl2 = 1.0 - st * t2
                of1 = st * (sq1 - r1 * (1.0 - t1))
                of2 = st * (sq2 - r2 * (1.0 - t2))
                for i, v in enumerate((sl1, sl2, of1, of2)):
                    terms[q, j, 4 * pb + i] = v
                co, si = cosine[pb], sine[pb]
                here = (sl1 * co, -sl1 * si, sl2 * si, sl2 * co, of1, of2)
                mm[pb] = here if mm[pb] is None else compose(here, mm[pb])
        for k in (1, 2, 4):
            mm = [compose(v, shifted(v, k)) for v in mm]
        for pb in range(2):
            before = shifted(mm[pb], 1)
            for i in range(6):
                seg[q, pb, i] = before[i]
                seg[q, pb, 6 + i] = lanes(mm[pb][i][7:8, :])

    for q in range(Q):
        scan_chunk(q)

    def chunk_total(q, pb):
        return tuple(seg[q, pb, 6 + i] for i in range(6))

    def rows_of(ref, pb):
        return tuple(lanes(ref[6 * pb + i : 6 * pb + i + 1, :]) for i in range(6))

    def keep(ref, pb, mm):
        for i in range(6):
            ref[6 * pb + i : 6 * pb + i + 1, :] = mm[i][0:1, :]

    for pb in range(2):
        whole = chunk_total(0, pb)
        for q in range(1, Q):
            whole = compose(chunk_total(q, pb), whole)
        keep(hbuf.at[c], pb, whole)

    half_copy = remote(hbuf.at[1 - LEAD], hbuf.at[1 - LEAD], h_sem.at[0], h_sem.at[1], partner)
    state_copy = remote(ebuf.at[1 - LEAD], ebuf.at[1 - LEAD], h_sem.at[2], h_sem.at[3], partner)

    def x_copy(dx):
        ref = xbuf.at[xi]
        target = dev(zi * NX + lax.rem(xi + dx, NX), m)
        return remote(ref, ref, x_send.at[dx], x_recv.at[xi], target)

    def x_arrival(k):
        return remote(xbuf.at[k], xbuf.at[k], x_send.at[0], x_recv.at[k], partner)

    def z_copy(dz):
        target = dev(lax.rem(zi + dz, NZ) * NX + xi, m)
        return remote(rowtot, zbuf.at[dz], z_send.at[dz], z_recv.at[dz], target)

    @pl.when(c != LEAD)
    def _():
        half_copy.start()

    @pl.when(c == LEAD)
    def _():
        @pl.when(xi < NX - 1)
        def _():
            pl.semaphore_wait(ready.at[1], NX - 1 - xi)

        @pl.when(zi < NZ - 1)
        def _():
            pl.semaphore_wait(ready.at[2], NZ - 1 - zi)

        half_copy.wait_recv()
        for pb in range(2):
            keep(xbuf.at[xi], pb, compose(rows_of(hbuf.at[1], pb), rows_of(hbuf.at[0], pb)))
        for dx in range(1, NX):
            x_copy(dx).start()
        for k in range(NX):

            @pl.when(xi != k)
            def _():
                x_arrival(k).wait_recv()

        partial = [[rows_of(xbuf.at[0], pb)] for pb in range(2)]
        for k in range(1, NX):
            for pb in range(2):
                partial[pb].append(compose(rows_of(xbuf.at[k], pb), partial[pb][-1]))
        for pb in range(2):
            keep(rowtot, pb, partial[pb][-1])

        for dz in range(1, NZ):

            @pl.when(zi + dz < NZ)
            def _():
                z_copy(dz).start()

        ahead = []
        for pb in range(2):
            before = identity
            for k in range(NX - 1):
                before = tuple(
                    jnp.where(xi == k + 1, v, w) for v, w in zip(partial[pb][k], before)
                )
            ahead.append(before)

        for dz in range(1, NZ):

            @pl.when(zi >= dz)
            def _():
                z_copy(dz).wait_recv()

        for pb in range(2):
            state = tuple(lanes(ini[pb, k : k + 1, :]) for k in range(2))
            for dz in range(NZ - 1, 0, -1):
                after = apply_map(rows_of(zbuf.at[dz], pb), state)
                state = tuple(jnp.where(zi >= dz, v, w) for v, w in zip(after, state))
            state = apply_map(ahead[pb], state)
            later = apply_map(rows_of(hbuf.at[0], pb), state)
            for k in range(2):
                at = 2 * pb + k
                ebuf[0, at : at + 1, :] = state[k][0:1, :]
                ebuf[1, at : at + 1, :] = later[k][0:1, :]
        state_copy.start()

    @pl.when(c != LEAD)
    def _():
        state_copy.wait_recv()

    current = {}
    for pb in range(2):
        state = tuple(lanes(ebuf[c, 2 * pb + k : 2 * pb + k + 1, :]) for k in range(2))
        for q in range(Q):
            current[q, pb] = apply_map(tuple(seg[q, pb, i] for i in range(6)), state)
            if q < Q - 1:
                state = apply_map(chunk_total(q, pb), state)

    pltpu.make_async_copy(wo.at[c], wo.at[c], wo_sem.at[0]).wait()
    wo_all = remote(wo.at[o], wo.at[o], wo_sem.at[1], wo_sem.at[2], partner)
    wo_all.wait_recv()

    def own(k, q):
        columns = 2 * k + q // 2
        h = lax.rem(q, 2)
        part = jnp.dot(stb[0, h], wo[0, columns], preferred_element_type=F32)
        return part + jnp.dot(stb[1, h], wo[1, columns], preferred_element_type=F32)

    def rs_copy(d, i):
        return remote(
            sbuf.at[d, i], rbuf.at[d, i], rs_send.at[0], rs_recv.at[d, i], (up, down)[d]
        )

    def last_copy(d, i):
        q = lax.rem(i + 2 * d, 4)
        h = lax.rem(q, 2)
        target = dev(s, 2 * ring(1 if d == 0 else -1) + q // 2)
        return remote(
            sbuf.at[d, i], fbuf.at[d, c, h], rs_send.at[0], f_recv.at[d, c, h], target
        )

    def item(d, i):
        dist = (17 - i) // 4
        return own(ring(dist) if d == 0 else ring(-dist), lax.rem(i + 2 * d, 4))

    def begin(i):
        for d in range(2):
            sbuf[d, i] = item(d, i).astype(BF16)
            rs_copy(d, i).start()

    for duo in ((0, 1), (2, 3)):
        chains = [(q, pb) for q in duo for pb in range(2)]
        pairs = {chain: ([], []) for chain in chains}
        for j in range(SEG):
            for q, pb in chains:
                x1, x2 = current[q, pb]
                u1 = cosine[pb] * x1 - sine[pb] * x2
                u2 = sine[pb] * x1 + cosine[pb] * x2
                x1 = terms[q, j, 4 * pb] * u1 + terms[q, j, 4 * pb + 2]
                x2 = terms[q, j, 4 * pb + 1] * u2 + terms[q, j, 4 * pb + 3]
                current[q, pb] = (x1, x2)
                at = 2 * (q * CH + j)
                nst[pb, pl.ds(at, 8, stride=2 * SEG), :] = x1
                nst[pb, pl.ds(at + 1, 8, stride=2 * SEG), :] = x2
                pairs[q, pb][0].append(x1)
                pairs[q, pb][1].append(x2)
                if j % 2 == 1:
                    for k in range(2):
                        both = jnp.concatenate(pairs[q, pb][k], axis=0).astype(BF16)
                        top = (q % 2) * CH + (j - 1) * 8
                        stb[pb, q // 2, top : top + 16, k * 128 : (k + 1) * 128] = both
                    pairs[q, pb] = ([], [])

        if duo == (0, 1):
            begin(0)

    @pl.loop(1, 4)
    def _(i):
        begin(i)

    def home(h):
        ref = nsb.at[pl.ds(pl.multiple_of(c * 2 * HALF, 2 * HALF), 2 * HALF)]
        if h == 0:
            return pltpu.make_async_copy(nst.at[c], ref, ns_sem.at[0])
        return remote(nst.at[o], ref, ns_sem.at[1], ns_sem.at[2], partner)

    home(0).start()
    home(1).start()

    def own_copy(h):
        return remote(pbuf.at[h], obuf.at[h], o_send.at[h], o_recv.at[h], partner)

    @pl.loop(4, 10)
    def _(i):
        for d in range(2):
            mine = item(d, i)
            rs_copy(d, i - 4).wait_recv()
            sbuf[d, i] = (mine + rbuf[d, i - 4].astype(F32)).astype(BF16)
            rs_copy(d, i).start()

        @pl.when(i < 6)
        def _():
            h = i - 4
            fin[h] = own(y, 2 * c + h)
            pbuf[h] = own(y, 2 * o + h).astype(BF16)
            own_copy(h).start()

    @pl.loop(10, STEPS)
    def _(i):
        for d in range(2):
            mine = item(d, i)
            rs_copy(d, i - 4).wait_recv()
            sbuf[d, i] = (mine + rbuf[d, i - 4].astype(F32)).astype(BF16)
            last_copy(d, i).start()

    def landed(d, core, h):
        ref = fbuf.at[d, core, h]
        return remote(ref, ref, rs_send.at[0], f_recv.at[d, core, h], partner)

    for h in range(2):
        own_copy(h).wait_recv()
        for mine in (True, False):
            core = c if mine else o
            base = fin[h] if mine else obuf[h].astype(F32)
            landed(o, core, h).wait_recv()
            fin[h if mine else 2 + h] = base + fbuf[o, core, h].astype(F32)
    for h in range(2):
        for mine in (True, False):
            core = c if mine else o
            landed(c, core, h).wait_recv()
            total = fin[h if mine else 2 + h] + fbuf[c, core, h].astype(F32)
            slot = 0 if mine else 1
            for u in range(TALL // CH):
                for j in range(SEG):
                    for k in range(2):
                        top = u * CH + j * 8
                        otmp[slot, k, pl.ds(u * CH + j, 8, stride=SEG), :] = total[
                            top : top + 8, k * 128 : (k + 1) * 128
                        ]
            r = pl.ds(pl.multiple_of(core * HALF + h * TALL, TALL), TALL)
            for k in range(2):
                outb[r, k * 128 : (k + 1) * 128] = otmp[slot, k].astype(BF16)

    def sent(ref, sem):
        remote(ref, ref, sem, rs_recv.at[0, 0], partner).wait_send()

    first.wait_send()
    for i in range(4):
        small_copy(i).wait_send()
    for core in range(2):

        @pl.when(c == core)
        def _():
            guess_to(1 - core).wait_send()

    @pl.when(s < NS - 1)
    def _():
        edge(c).wait_send()

    sent(xg.at[pl.ds(0, 14)], ag_send.at[0])
    sent(wi.at[c], wi_send.at[0])
    wo_all.wait_send()

    @pl.when(c != LEAD)
    def _():
        half_copy.wait_send()

    @pl.when(c == LEAD)
    def _():
        state_copy.wait_send()
        for dx in range(1, NX):
            x_copy(dx).wait_send()
        for dz in range(1, NZ):

            @pl.when(zi + dz < NZ)
            def _():
                z_copy(dz).wait_send()

    home(0).wait()
    home(1).wait_send()
    other_half = nsb.at[pl.ds(pl.multiple_of(o * 2 * HALF, 2 * HALF), 2 * HALF)]
    remote(nst.at[o], other_half, ns_sem.at[1], ns_sem.at[2], partner).wait_recv()
    for h in range(2):
        own_copy(h).wait_send()
    sent(sbuf, rs_send.at[0])


def write_out(state, out, state_hbm, out_hbm, sem):
    copies = (
        pltpu.make_async_copy(state, state_hbm, sem.at[0]),
        pltpu.make_async_copy(out, out_hbm, sem.at[1]),
    )
    for copy in copies:
        copy.start()
    for copy in copies:
        copy.wait()


def local(inputs, guess, initial, w_in, bias, angle, strength, w_out):
    dma = pltpu.SemaphoreType.DMA
    hbm = pl.BlockSpec(memory_space=pltpu.HBM)
    vmem = pl.BlockSpec(memory_space=pltpu.VMEM)
    new_state, output = pl.pallas_call(
        kernel,
        out_shape=(
            jax.ShapeDtypeStruct((2 * ROWS, 128), F32),
            jax.ShapeDtypeStruct((ROWS, BLK), BF16),
        ),
        in_specs=[hbm] * 8,
        out_specs=(vmem, vmem),
        scratch_shapes=[
            pltpu.VMEM((16, HALF, BLK), BF16),
            pltpu.VMEM((8192, 128), BF16),
            pltpu.VMEM((2, 16, BLK, BLK), BF16),
            pltpu.VMEM((2 * BLK, 128), F32),
            pltpu.VMEM((2, 16, BLK, BLK), BF16),
            pltpu.VMEM((4, HALF, 128), F32),
            pltpu.VMEM((2, 8 + 2 * HALF, 128), F32),
            pltpu.VMEM((Q, SEG, 4, 8, 128), F32),
            pltpu.VMEM((Q, SEG, 8, 8, 128), F32),
            pltpu.VMEM((Q, 2, 12, 8, 128), F32),
            pltpu.VMEM((2, 12, 128), F32),
            pltpu.VMEM((2, 8, 128), F32),
            pltpu.VMEM((NX, 12, 128), F32),
            pltpu.VMEM((12, 128), F32),
            pltpu.VMEM((NZ, 12, 128), F32),
            pltpu.VMEM((2, 2 * HALF, 128), F32),
            pltpu.VMEM((2, 2, TALL, BLK), BF16),
            pltpu.VMEM((2, STEPS, TALL, BLK), BF16),
            pltpu.VMEM((2, 10, TALL, BLK), BF16),
            pltpu.VMEM((2, 2, 2, TALL, BLK), BF16),
            pltpu.VMEM((2, TALL, BLK), BF16),
            pltpu.VMEM((2, TALL, BLK), BF16),
            pltpu.VMEM((4, TALL, BLK), F32),
            pltpu.VMEM((2, 2, TALL, 128), F32),
            pltpu.VMEM((2, 2, 128), F32),
            pltpu.VMEM((2, 2, 128), F32),
            pltpu.VMEM((2, 1, 128), F32),
            pltpu.VMEM((2, 1, 128), F32),
            dma((7,)),
            dma((4,)),
            dma((4,)),
            dma((2,)),
            dma((2, 3, 4)),
            dma((2, 6)),
            dma((1,)),
            dma((1,)),
            dma((16,)),
            dma((2,)),
            dma((1,)),
            dma((2,)),
            dma((3,)),
            dma((4,)),
            dma((NX,)),
            dma((NX,)),
            dma((NZ,)),
            dma((NZ,)),
            dma((3,)),
            dma((2,)),
            dma((2,)),
            dma((1,)),
            dma((2, 10)),
            dma((2, 2, 2)),
            pltpu.SemaphoreType.REGULAR((3,)),
        ],
        compiler_params=pltpu.CompilerParams(
            collective_id=0, has_side_effects=True, vmem_limit_bytes=48 * 1024 * 1024
        ),
    )(*(pltpu.with_memory_space_constraint(v, pltpu.HBM) for v in (
        inputs,
        guess.reshape(2 * ROWS, 128),
        initial,
        w_in.reshape(8192, 128),
        bias,
        angle.reshape(1, 128),
        strength.reshape(1, 128),
        w_out.reshape(BLK, 4096),
    )))
    new_state, output = pl.pallas_call(
        write_out,
        out_shape=(
            jax.ShapeDtypeStruct((2 * ROWS, 128), F32),
            jax.ShapeDtypeStruct((ROWS, BLK), BF16),
        ),
        in_specs=[pl.BlockSpec(memory_space=pl.ANY)] * 2,
        out_specs=(hbm, hbm),
        scratch_shapes=[dma((2,))],
        compiler_params=pltpu.CompilerParams(vmem_limit_bytes=4 * 1024 * 1024),
    )(new_state, output)
    return new_state.reshape(ROWS, 2, 128), output


def solution(mesh):
    placed = (
        P("seq", "mp"),
        P("seq", None, "mp"),
        P(None, "mp"),
        P(None, None, "mp"),
        P(None, "mp"),
        P("mp"),
        P("mp"),
        P(None, "mp", None),
    )
    return jax.shard_map(
        local,
        mesh=mesh,
        in_specs=placed,
        out_specs=(P("seq", None, "mp"), P("seq", "mp")),
        check_vma=False,
    )
```

```python
import jax
import jax.numpy as jnp
from jax import lax
from jax.experimental import pallas as pl
from jax.experimental.pallas import tpu as pltpu
from jax.sharding import PartitionSpec as P

MESH = pl.DeviceIdType.MESH
F32 = jnp.float32
BF16 = jnp.bfloat16

NY = 8
NX = 4
NZ = 8
NS = NX * NZ
ROWS = 512
BLK = 256
HALF = ROWS // 2
TALL = HALF // 2
Q = 4
CH = HALF // Q
SEG = CH // 8
LEAD = 1
STEPS = 14


def compose(later, earlier):
    a, b, c, d, e, f = later
    p, q, r, s, t, u = earlier
    return (
        a * p + b * r,
        a * q + b * s,
        c * p + d * r,
        c * q + d * s,
        a * t + b * u + e,
        c * t + d * u + f,
    )


def apply_map(m, state):
    a, b, c, d, e, f = m
    x, y = state
    return (a * x + b * y + e, c * x + d * y + f)


def kernel(
    x_hbm,
    g_hbm,
    init_hbm,
    w_hbm,
    bias_hbm,
    ang_hbm,
    str_hbm,
    wo_hbm,
    nsb,
    outb,
    xg,
    w2,
    wi,
    wtmp,
    wo,
    acc,
    gs,
    rot,
    terms,
    seg,
    hbuf,
    ebuf,
    xbuf,
    rowtot,
    zbuf,
    nst,
    stb,
    sbuf,
    rbuf,
    fbuf,
    pbuf,
    obuf,
    fin,
    otmp,
    ini,
    bia,
    ang,
    stg,
    loc_sem,
    small_send,
    small_recv,
    first_sem,
    ag_recv,
    far_recv,
    ag_send,
    wi_send,
    wi_recv,
    g_sem,
    e_send,
    e_recv,
    wo_sem,
    h_sem,
    x_send,
    x_recv,
    z_send,
    z_recv,
    ns_sem,
    o_send,
    o_recv,
    rs_send,
    rs_recv,
    f_recv,
    ready,
):
    s = lax.axis_index("seq")
    m = lax.axis_index("mp")
    y = m // 2
    c = m % 2
    zi = s // NX
    xi = s % NX

    def ring(k):
        return lax.rem(y + k + 2 * NY, NY)

    def dev(seq, mp):
        return {"seq": seq, "mp": mp}

    def remote(src, dst, send, recv, target):
        return pltpu.make_async_remote_copy(
            src_ref=src,
            dst_ref=dst,
            send_sem=send,
            recv_sem=recv,
            device_id=target,
            device_id_type=MESH,
        )

    o = 1 - c
    other = 2 * y + o
    up = dev(s, ring(1) * 2 + c)
    down = dev(s, ring(-1) * 2 + c)
    partner = dev(s, other)

    barrier = pltpu.get_barrier_semaphore()

    def greet(target):
        pl.semaphore_signal(barrier, inc=1, device_id=target, device_id_type=MESH)

    greet(partner)
    for core in range(2):
        greet(dev(s, ring(1) * 2 + core))
        greet(dev(s, ring(-1) * 2 + core))

    def half_rows(core):
        return pl.ds(pl.multiple_of(core * HALF, HALF), HALF)

    in_copy = pltpu.make_async_copy(x_hbm.at[half_rows(c)], xg.at[m], loc_sem.at[0])
    in_copy.start()
    w_copy = pltpu.make_async_copy(w_hbm, w2, loc_sem.at[1])
    w_copy.start()
    small = ((init_hbm, ini), (bias_hbm, bia), (ang_hbm, ang), (str_hbm, stg))
    small_copies = [
        pltpu.make_async_copy(a, b.at[c], loc_sem.at[2 + i]) for i, (a, b) in enumerate(small)
    ]
    for copy in small_copies:
        copy.start()

    for dx in range(1, NX):

        @pl.when((xi + dx < NX) & (c == LEAD))
        def _():
            greet(dev(s + dx, m))

    for dz in range(1, NZ):

        @pl.when((zi + dz < NZ) & (c == LEAD))
        def _():
            greet(dev(s + dz * NX, m))

    @pl.when(s < NS - 1)
    def _():
        greet(dev(s + 1, 2 * y))

    pl.semaphore_wait(barrier, 5 + (c if LEAD == 1 else o) * (xi + zi) + 2 * (lax.min(s, 1) * o))

    def answer(sem, target):
        pl.semaphore_signal(sem, inc=1, device_id=target, device_id_type=MESH)

    def block_of(pos, a):
        return 2 * pos + jnp.where(a < 2, c, o)

    def tall(h):
        return pl.ds(pl.multiple_of(h * TALL, TALL), TALL)

    def ici(pos, a, g, d):
        ref = xg.at[block_of(pos, a), tall(lax.rem(a, 2))]
        return remote(ref, ref, ag_send.at[0], ag_recv.at[d, g, a], (up, down)[d])

    def far_piece(pos, slot, d):
        columns = pl.ds(d * 128, 128)
        if slot < 2:
            ref = xg.at[2 * pos + c, pl.ds(slot * TALL, TALL), columns]
        else:
            ref = xg.at[2 * pos + o, pl.ds((slot - 2) * CH, CH), columns]
        return remote(ref, ref, ag_send.at[0], far_recv.at[d, slot], (up, down)[d])

    first = remote(
        x_hbm.at[half_rows(o)], xg.at[m], first_sem.at[0], first_sem.at[1], partner
    )
    first.start()
    in_copy.wait()
    for a in range(2):
        for d in range(2):
            ici(y, a, 0, d).start()

    def small_copy(i):
        a, b = small[i]
        return remote(a, b.at[c], small_send.at[i], small_recv.at[i], partner)

    for i in range(4):
        small_copy(i).start()

    @pl.when((s > 0) & (c == 0))
    def _():
        answer(ready.at[0], dev(s - 1, 2 * y))
        answer(ready.at[0], dev(s - 1, 2 * y + 1))

    for dx in range(1, NX):

        @pl.when((xi >= dx) & (c == LEAD))
        def _():
            answer(ready.at[1], dev(s - dx, m))

    for dz in range(1, NZ):

        @pl.when((zi >= dz) & (c == LEAD))
        def _():
            answer(ready.at[2], dev(s - dz * NX, m))

    def guess_own(core):
        if core == 0:
            return pltpu.make_async_copy(
                g_hbm.at[pl.ds(0, 2 * HALF)], gs.at[0, pl.ds(8, 2 * HALF)], loc_sem.at[6]
            )
        return pltpu.make_async_copy(
            g_hbm.at[pl.ds(2 * HALF - 8, 2 * HALF + 8)], gs.at[1], loc_sem.at[6]
        )

    def guess_to(core):
        pb = 1 - core
        if core == 0:
            return remote(
                g_hbm.at[pl.ds(0, 2 * HALF)],
                gs.at[pb, pl.ds(8, 2 * HALF)],
                g_sem.at[0],
                g_sem.at[1],
                partner,
            )
        return remote(
            g_hbm.at[pl.ds(2 * HALF - 8, 2 * HALF + 8)],
            gs.at[pb],
            g_sem.at[0],
            g_sem.at[1],
            partner,
        )

    first.wait_recv()
    for a in range(2, 4):
        for d in range(2):
            ici(y, a, 0, d).start()
    w_copy.wait()

    def prepare(b):
        wtmp[...] = w2[pl.ds(pl.multiple_of(b * 2 * BLK, 2 * BLK), 2 * BLK), :].astype(F32)
        for k in range(2):
            wi[c, b, :, k * 128 : (k + 1) * 128] = wtmp[pl.ds(k, BLK, stride=2), :].astype(BF16)
        wi_copy(c, b).start()

    def wi_copy(pb, b):
        return remote(wi.at[pb, b], wi.at[pb, b], wi_send.at[0], wi_recv.at[b], partner)

    prepare(m)
    prepare(other)

    for core in range(2):

        @pl.when(c == core)
        def _():
            guess_own(core).start()
            guess_to(1 - core).start()

    far = ring(4)
    prepare(2 * far)
    prepare(2 * far + 1)

    for copy in small_copies:
        copy.wait()
    for i in range(4):
        small_copy(i).wait_recv()

    def lanes(v):
        return jnp.broadcast_to(v, (8, 128))

    cosine = [lanes(jnp.cos(ang[pb])) for pb in range(2)]
    sine = [lanes(jnp.sin(ang[pb])) for pb in range(2)]
    strength = [lanes(stg[pb]) for pb in range(2)]

    def products(b, r):
        lhs = xg[b, r, :]
        return [jnp.dot(lhs, wi[pb, b], preferred_element_type=F32) for pb in range(2)]

    def start_group(h):
        r = tall(h)

        @pl.when(h == 0)
        def _():
            wi_copy(o, m).wait_recv()
            wi_copy(o, other).wait_recv()

        one = products(m, r)
        two = products(other, r)
        for pb in range(2):
            part = one[pb] + two[pb]
            acc[2 * pb, r, :] = part[:, :128] + bia[pb, 0:1, :]
            acc[2 * pb + 1, r, :] = part[:, 128:] + bia[pb, 1:2, :]

    def add_blocks(blocks, r):
        part = None
        for b in blocks:
            term = products(b, r)
            part = term if part is None else [u + v for u, v in zip(part, term)]
        for pb in range(2):
            acc[2 * pb, r, :] += part[pb][:, :128]
            acc[2 * pb + 1, r, :] += part[pb][:, 128:]

    def add_group(g, h):
        blocks = [2 * ring(k) + core for k in (-g, g) for core in range(2)]

        def weights():
            for b in blocks:
                wi_copy(o, b).wait_recv()

        if isinstance(h, int):
            if h == 0:
                weights()
            add_blocks(blocks, pl.ds(h * TALL, TALL))
        else:
            pl.when(h == 0)(weights)
            add_blocks(blocks, tall(h))

    def rotate_guess(q):
        @pl.loop(0, SEG)
        def _(j):
            at = 6 + 2 * (q * CH + j)
            for pb in range(2):
                one = gs[pb, pl.ds(at, 8, stride=2 * SEG), :]
                two = gs[pb, pl.ds(at + 1, 8, stride=2 * SEG), :]
                rot[q, j, 2 * pb] = cosine[pb] * one - sine[pb] * two
                rot[q, j, 2 * pb + 1] = sine[pb] * one + cosine[pb] * two

    def prepare_group(g, i):
        prepare(2 * ring(jnp.where(i < 2, -g, g)) + lax.rem(i, 2))

    def edge(pb):
        return remote(
            g_hbm.at[pl.ds(2 * ROWS - 8, 8)],
            gs.at[pb, pl.ds(0, 8)],
            e_send.at[0],
            e_recv.at[pb],
            dev(lax.rem(s + 1, NS), 2 * y),
        )

    def wo_cols(k):
        return wo_hbm.at[:, pl.ds(k * BLK, BLK)]

    def wo_copy(k):
        return remote(wo_cols(k), wo.at[c, k], wo_sem.at[1], wo_sem.at[2], partner)

    for g in range(1, 4):
        if g == 2:
            for k in range(2 * NY):
                pltpu.make_async_copy(wo_cols(k), wo.at[c, k], wo_sem.at[0]).start()
                wo_copy(k).start()

            @pl.when(s < NS - 1)
            def _():
                pl.semaphore_wait(ready.at[0], 1)
                edge(c).start()

        if g == 3:
            for core in range(2):

                @pl.when(c == core)
                def _():
                    guess_own(core).wait()
                    guess_to(core).wait_recv()

            @pl.when((s > 0) & (c == 0))
            def _():
                for pb in range(2):
                    edge(pb).wait_recv()

            @pl.when((s == 0) & (c == 0))
            def _():
                for pb in range(2):
                    gs[pb, 6:8, :] = ini[pb]

            for a in range(4):
                for d in range(2):
                    pos = ring(-3 if d == 0 else 3)
                    ici(pos, a, 2, d).wait_recv()
                    for slot in ((0,), (1,), (2, 3), (4, 5))[a]:
                        far_piece(pos, slot, d).start()
                if a < 2:
                    add_group(2, a)
                if a == 3:
                    add_group(3, 0)
                rotate_guess(a)
        else:

            @pl.loop(0, 4)
            def _(a):
                for d in range(2):
                    pos = ring(-g if d == 0 else g)
                    ici(pos, a, g - 1, d).wait_recv()
                    ici(pos, a, g, d).start()
                if g == 1:
                    prepare_group(1, a)
                    prepare_group(2, a)
                else:
                    prepare_group(3, a)

                @pl.when(lax.rem(a, 2) == 1)
                def _():
                    if g == 1:
                        start_group(a // 2)
                    else:
                        add_group(1, a // 2)

    iota = lax.broadcasted_iota(jnp.int32, (8, 128), 0)
    one_v = jnp.ones((8, 128), F32)
    zero_v = jnp.zeros((8, 128), F32)
    identity = (one_v, zero_v, zero_v, one_v, zero_v, zero_v)

    def shifted(mm, k):
        return tuple(
            jnp.where(iota < k, ident, pltpu.roll(v, k, 0)) for v, ident in zip(mm, identity)
        )

    def scan_chunk(q):
        for d in range(2):
            for slot in ((0, 2), (3,), (1, 4), (5,))[q]:
                far_piece(far, slot, d).wait_recv()
        if q == 0:
            add_group(3, 1)
            wi_copy(o, 2 * far).wait_recv()
            wi_copy(o, 2 * far + 1).wait_recv()
        add_blocks((2 * far, 2 * far + 1), pl.ds(q * CH, CH))
        mm = [None, None]
        for j in range(SEG):
            at = q * CH + j
            for pb in range(2):
                st = strength[pb]
                r1 = rot[q, j, 2 * pb]
                r2 = rot[q, j, 2 * pb + 1]
                sq1 = jnp.tanh(r1 + acc[2 * pb, pl.ds(at, 8, stride=SEG), :])
                sq2 = jnp.tanh(r2 + acc[2 * pb + 1, pl.ds(at, 8, stride=SEG), :])
                t1 = sq1 * sq1
                t2 = sq2 * sq2
                sl1 = 1.0 - st * t1
                sl2 = 1.0 - st * t2
                of1 = st * (sq1 - r1 * (1.0 - t1))
                of2 = st * (sq2 - r2 * (1.0 - t2))
                for i, v in enumerate((sl1, sl2, of1, of2)):
                    terms[q, j, 4 * pb + i] = v
                co, si = cosine[pb], sine[pb]
                here = (sl1 * co, -sl1 * si, sl2 * si, sl2 * co, of1, of2)
                mm[pb] = here if mm[pb] is None else compose(here, mm[pb])
        for k in (1, 2, 4):
            mm = [compose(v, shifted(v, k)) for v in mm]
        for pb in range(2):
            before = shifted(mm[pb], 1)
            for i in range(6):
                seg[q, pb, i] = before[i]
                seg[q, pb, 6 + i] = lanes(mm[pb][i][7:8, :])

    for q in range(Q):
        scan_chunk(q)

    def chunk_total(q, pb):
        return tuple(seg[q, pb, 6 + i] for i in range(6))

    def rows_of(ref, pb):
        return tuple(lanes(ref[6 * pb + i : 6 * pb + i + 1, :]) for i in range(6))

    def keep(ref, pb, mm):
        for i in range(6):
            ref[6 * pb + i : 6 * pb + i + 1, :] = mm[i][0:1, :]

    for pb in range(2):
        whole = chunk_total(0, pb)
        for q in range(1, Q):
            whole = compose(chunk_total(q, pb), whole)
        keep(hbuf.at[c], pb, whole)

    half_copy = remote(hbuf.at[1 - LEAD], hbuf.at[1 - LEAD], h_sem.at[0], h_sem.at[1], partner)
    state_copy = remote(ebuf.at[1 - LEAD], ebuf.at[1 - LEAD], h_sem.at[2], h_sem.at[3], partner)

    def x_copy(dx):
        ref = xbuf.at[xi]
        target = dev(zi * NX + lax.rem(xi + dx, NX), m)
        return remote(ref, ref, x_send.at[dx], x_recv.at[xi], target)

    def x_arrival(k):
        return remote(xbuf.at[k], xbuf.at[k], x_send.at[0], x_recv.at[k], partner)

    def z_copy(dz):
        target = dev(lax.rem(zi + dz, NZ) * NX + xi, m)
        return remote(rowtot, zbuf.at[dz], z_send.at[dz], z_recv.at[dz], target)

    @pl.when(c != LEAD)
    def _():
        half_copy.start()

    @pl.when(c == LEAD)
    def _():
        @pl.when(xi < NX - 1)
        def _():
            pl.semaphore_wait(ready.at[1], NX - 1 - xi)

        @pl.when(zi < NZ - 1)
        def _():
            pl.semaphore_wait(ready.at[2], NZ - 1 - zi)

        half_copy.wait_recv()
        for pb in range(2):
            keep(xbuf.at[xi], pb, compose(rows_of(hbuf.at[1], pb), rows_of(hbuf.at[0], pb)))
        for dx in (2, 1, 3):
            x_copy(dx).start()
        for k in range(NX):

            @pl.when(xi != k)
            def _():
                x_arrival(k).wait_recv()

        partial = [[rows_of(xbuf.at[0], pb)] for pb in range(2)]
        for k in range(1, NX):
            for pb in range(2):
                partial[pb].append(compose(rows_of(xbuf.at[k], pb), partial[pb][-1]))
        for pb in range(2):
            keep(rowtot, pb, partial[pb][-1])

        for dz in (4, 3, 5, 2, 6, 1, 7):

            @pl.when(zi + dz < NZ)
            def _():
                z_copy(dz).start()

        ahead = []
        for pb in range(2):
            before = identity
            for k in range(NX - 1):
                before = tuple(
                    jnp.where(xi == k + 1, v, w) for v, w in zip(partial[pb][k], before)
                )
            ahead.append(before)

        for dz in range(1, NZ):

            @pl.when(zi >= dz)
            def _():
                z_copy(dz).wait_recv()

        for pb in range(2):
            state = tuple(lanes(ini[pb, k : k + 1, :]) for k in range(2))
            for dz in range(NZ - 1, 0, -1):
                after = apply_map(rows_of(zbuf.at[dz], pb), state)
                state = tuple(jnp.where(zi >= dz, v, w) for v, w in zip(after, state))
            state = apply_map(ahead[pb], state)
            later = apply_map(rows_of(hbuf.at[0], pb), state)
            for k in range(2):
                at = 2 * pb + k
                ebuf[0, at : at + 1, :] = state[k][0:1, :]
                ebuf[1, at : at + 1, :] = later[k][0:1, :]
        state_copy.start()

    @pl.when(c != LEAD)
    def _():
        state_copy.wait_recv()

    current = {}
    for pb in range(2):
        state = tuple(lanes(ebuf[c, 2 * pb + k : 2 * pb + k + 1, :]) for k in range(2))
        for q in range(Q):
            current[q, pb] = apply_map(tuple(seg[q, pb, i] for i in range(6)), state)
            if q < Q - 1:
                state = apply_map(chunk_total(q, pb), state)

    pltpu.make_async_copy(wo.at[c], wo.at[c], wo_sem.at[0]).wait()
    wo_all = remote(wo.at[o], wo.at[o], wo_sem.at[1], wo_sem.at[2], partner)
    wo_all.wait_recv()

    def own(k, q):
        columns = 2 * k + q // 2
        h = lax.rem(q, 2)
        part = jnp.dot(stb[0, h], wo[0, columns], preferred_element_type=F32)
        return part + jnp.dot(stb[1, h], wo[1, columns], preferred_element_type=F32)

    def rs_copy(d, i):
        return remote(
            sbuf.at[d, i], rbuf.at[d, i], rs_send.at[0], rs_recv.at[d, i], (up, down)[d]
        )

    def last_copy(d, i):
        q = lax.rem(i + 2 * d, 4)
        h = lax.rem(q, 2)
        target = dev(s, 2 * ring(1 if d == 0 else -1) + q // 2)
        return remote(
            sbuf.at[d, i], fbuf.at[d, c, h], rs_send.at[0], f_recv.at[d, c, h], target
        )

    def item(d, i):
        dist = (17 - i) // 4
        return own(ring(dist) if d == 0 else ring(-dist), lax.rem(i + 2 * d, 4))

    def begin(i):
        for d in range(2):
            sbuf[d, i] = item(d, i).astype(BF16)
            rs_copy(d, i).start()

    for duo in ((0, 1), (2, 3)):
        chains = [(q, pb) for q in duo for pb in range(2)]
        pairs = {chain: ([], []) for chain in chains}
        for j in range(SEG):
            for q, pb in chains:
                x1, x2 = current[q, pb]
                u1 = cosine[pb] * x1 - sine[pb] * x2
                u2 = sine[pb] * x1 + cosine[pb] * x2
                x1 = terms[q, j, 4 * pb] * u1 + terms[q, j, 4 * pb + 2]
                x2 = terms[q, j, 4 * pb + 1] * u2 + terms[q, j, 4 * pb + 3]
                current[q, pb] = (x1, x2)
                at = 2 * (q * CH + j)
                nst[pb, pl.ds(at, 8, stride=2 * SEG), :] = x1
                nst[pb, pl.ds(at + 1, 8, stride=2 * SEG), :] = x2
                pairs[q, pb][0].append(x1)
                pairs[q, pb][1].append(x2)
                if j % 2 == 1:
                    for k in range(2):
                        both = jnp.concatenate(pairs[q, pb][k], axis=0).astype(BF16)
                        top = (q % 2) * CH + (j - 1) * 8
                        stb[pb, q // 2, top : top + 16, k * 128 : (k + 1) * 128] = both
                    pairs[q, pb] = ([], [])

        if duo == (0, 1):
            begin(0)

    @pl.loop(1, 4)
    def _(i):
        begin(i)

    def home(h):
        ref = nsb.at[pl.ds(pl.multiple_of(c * 2 * HALF, 2 * HALF), 2 * HALF)]
        if h == 0:
            return pltpu.make_async_copy(nst.at[c], ref, ns_sem.at[0])
        return remote(nst.at[o], ref, ns_sem.at[1], ns_sem.at[2], partner)

    home(0).start()
    home(1).start()

    def own_copy(h):
        return remote(pbuf.at[h], obuf.at[h], o_send.at[h], o_recv.at[h], partner)

    @pl.loop(4, 10)
    def _(i):
        for d in range(2):
            mine = item(d, i)
            rs_copy(d, i - 4).wait_recv()
            sbuf[d, i] = (mine + rbuf[d, i - 4].astype(F32)).astype(BF16)
            rs_copy(d, i).start()

        @pl.when(i < 6)
        def _():
            h = i - 4
            fin[h] = own(y, 2 * c + h)
            pbuf[h] = own(y, 2 * o + h).astype(BF16)
            own_copy(h).start()

    @pl.loop(10, STEPS)
    def _(i):
        for d in range(2):
            mine = item(d, i)
            rs_copy(d, i - 4).wait_recv()
            sbuf[d, i] = (mine + rbuf[d, i - 4].astype(F32)).astype(BF16)
            last_copy(d, i).start()

    def landed(d, core, h):
        ref = fbuf.at[d, core, h]
        return remote(ref, ref, rs_send.at[0], f_recv.at[d, core, h], partner)

    for h in range(2):
        own_copy(h).wait_recv()
        for mine in (True, False):
            core = c if mine else o
            base = fin[h] if mine else obuf[h].astype(F32)
            landed(o, core, h).wait_recv()
            fin[h if mine else 2 + h] = base + fbuf[o, core, h].astype(F32)
    for h in range(2):
        for mine in (True, False):
            core = c if mine else o
            landed(c, core, h).wait_recv()
            total = fin[h if mine else 2 + h] + fbuf[c, core, h].astype(F32)
            slot = 0 if mine else 1
            for u in range(TALL // CH):
                for j in range(SEG):
                    for k in range(2):
                        top = u * CH + j * 8
                        otmp[slot, k, pl.ds(u * CH + j, 8, stride=SEG), :] = total[
                            top : top + 8, k * 128 : (k + 1) * 128
                        ]
            r = pl.ds(pl.multiple_of(core * HALF + h * TALL, TALL), TALL)
            for k in range(2):
                outb[r, k * 128 : (k + 1) * 128] = otmp[slot, k].astype(BF16)

    def sent(ref, sem):
        remote(ref, ref, sem, rs_recv.at[0, 0], partner).wait_send()

    first.wait_send()
    for i in range(4):
        small_copy(i).wait_send()
    for core in range(2):

        @pl.when(c == core)
        def _():
            guess_to(1 - core).wait_send()

    @pl.when(s < NS - 1)
    def _():
        edge(c).wait_send()

    sent(xg.at[pl.ds(0, 14)], ag_send.at[0])
    sent(wi.at[c], wi_send.at[0])
    wo_all.wait_send()

    @pl.when(c != LEAD)
    def _():
        half_copy.wait_send()

    @pl.when(c == LEAD)
    def _():
        state_copy.wait_send()
        for dx in range(1, NX):
            x_copy(dx).wait_send()
        for dz in range(1, NZ):

            @pl.when(zi + dz < NZ)
            def _():
                z_copy(dz).wait_send()

    home(0).wait()
    home(1).wait_send()
    other_half = nsb.at[pl.ds(pl.multiple_of(o * 2 * HALF, 2 * HALF), 2 * HALF)]
    remote(nst.at[o], other_half, ns_sem.at[1], ns_sem.at[2], partner).wait_recv()
    for h in range(2):
        own_copy(h).wait_send()
    sent(sbuf, rs_send.at[0])


def write_out(state, out, state_hbm, out_hbm, sem):
    copies = (
        pltpu.make_async_copy(state, state_hbm, sem.at[0]),
        pltpu.make_async_copy(out, out_hbm, sem.at[1]),
    )
    for copy in copies:
        copy.start()
    for copy in copies:
        copy.wait()


def local(inputs, guess, initial, w_in, bias, angle, strength, w_out):
    dma = pltpu.SemaphoreType.DMA
    hbm = pl.BlockSpec(memory_space=pltpu.HBM)
    vmem = pl.BlockSpec(memory_space=pltpu.VMEM)
    new_state, output = pl.pallas_call(
        kernel,
        out_shape=(
            jax.ShapeDtypeStruct((2 * ROWS, 128), F32),
            jax.ShapeDtypeStruct((ROWS, BLK), BF16),
        ),
        in_specs=[hbm] * 8,
        out_specs=(vmem, vmem),
        scratch_shapes=[
            pltpu.VMEM((16, HALF, BLK), BF16),
            pltpu.VMEM((8192, 128), BF16),
            pltpu.VMEM((2, 16, BLK, BLK), BF16),
            pltpu.VMEM((2 * BLK, 128), F32),
            pltpu.VMEM((2, 16, BLK, BLK), BF16),
            pltpu.VMEM((4, HALF, 128), F32),
            pltpu.VMEM((2, 8 + 2 * HALF, 128), F32),
            pltpu.VMEM((Q, SEG, 4, 8, 128), F32),
            pltpu.VMEM((Q, SEG, 8, 8, 128), F32),
            pltpu.VMEM((Q, 2, 12, 8, 128), F32),
            pltpu.VMEM((2, 12, 128), F32),
            pltpu.VMEM((2, 8, 128), F32),
            pltpu.VMEM((NX, 12, 128), F32),
            pltpu.VMEM((12, 128), F32),
            pltpu.VMEM((NZ, 12, 128), F32),
            pltpu.VMEM((2, 2 * HALF, 128), F32),
            pltpu.VMEM((2, 2, TALL, BLK), BF16),
            pltpu.VMEM((2, STEPS, TALL, BLK), BF16),
            pltpu.VMEM((2, 10, TALL, BLK), BF16),
            pltpu.VMEM((2, 2, 2, TALL, BLK), BF16),
            pltpu.VMEM((2, TALL, BLK), BF16),
            pltpu.VMEM((2, TALL, BLK), BF16),
            pltpu.VMEM((4, TALL, BLK), F32),
            pltpu.VMEM((2, 2, TALL, 128), F32),
            pltpu.VMEM((2, 2, 128), F32),
            pltpu.VMEM((2, 2, 128), F32),
            pltpu.VMEM((2, 1, 128), F32),
            pltpu.VMEM((2, 1, 128), F32),
            dma((7,)),
            dma((4,)),
            dma((4,)),
            dma((2,)),
            dma((2, 3, 4)),
            dma((2, 6)),
            dma((1,)),
            dma((1,)),
            dma((16,)),
            dma((2,)),
            dma((1,)),
            dma((2,)),
            dma((3,)),
            dma((4,)),
            dma((NX,)),
            dma((NX,)),
            dma((NZ,)),
            dma((NZ,)),
            dma((3,)),
            dma((2,)),
            dma((2,)),
            dma((1,)),
            dma((2, 10)),
            dma((2, 2, 2)),
            pltpu.SemaphoreType.REGULAR((3,)),
        ],
        compiler_params=pltpu.CompilerParams(
            collective_id=0, has_side_effects=True, vmem_limit_bytes=48 * 1024 * 1024
        ),
    )(*(pltpu.with_memory_space_constraint(v, pltpu.HBM) for v in (
        inputs,
        guess.reshape(2 * ROWS, 128),
        initial,
        w_in.reshape(8192, 128),
        bias,
        angle.reshape(1, 128),
        strength.reshape(1, 128),
        w_out.reshape(BLK, 4096),
    )))
    new_state, output = pl.pallas_call(
        write_out,
        out_shape=(
            jax.ShapeDtypeStruct((2 * ROWS, 128), F32),
            jax.ShapeDtypeStruct((ROWS, BLK), BF16),
        ),
        in_specs=[pl.BlockSpec(memory_space=pl.ANY)] * 2,
        out_specs=(hbm, hbm),
        scratch_shapes=[dma((2,))],
        compiler_params=pltpu.CompilerParams(vmem_limit_bytes=4 * 1024 * 1024),
    )(new_state, output)
    return new_state.reshape(ROWS, 2, 128), output


def solution(mesh):
    placed = (
        P("seq", "mp"),
        P("seq", None, "mp"),
        P(None, "mp"),
        P(None, None, "mp"),
        P(None, "mp"),
        P("mp"),
        P("mp"),
        P(None, "mp", None),
    )
    return jax.shard_map(
        local,
        mesh=mesh,
        in_specs=placed,
        out_specs=(P("seq", None, "mp"), P("seq", "mp")),
        check_vma=False,
    )
```
